32 devices in a mesh: row: 2 (over y), col: 4 (over x, core), rep: 4 (over z).
Axes of the slice: x: 2, y: 2, z: 4, core: 2. Of those that a mesh axis runs over, the one named last changes fastest.
Arguments:
- hidden: bfloat16 [512, 7168], P('rep'), may hold values from -6 to 6
- train_weight: bfloat16 [7168, 16384], P(('rep', 'row'), 'col'), may hold values from -0.0625 to 0.0625
- shard_order: int32 [4, 4, 2], replicated, may hold values from 0 to 1, each once within a row
Outputs:
- served_weight: bfloat16 [7168, 16384], P(None, ('col', 'row'))
- projected: float32 [512, 16384], P('rep', ('col', 'row'))
The draws below stay inside these ranges and needn't reach their ends.
Inputs may be any that keep to these rules, and one draw needn't show every extreme that they name: Each shard_order[c, k] is a permutation of 0 to 1.
All inputs are finite; a program needn't handle non-finite values.
Results may differ from the reference program's by a relative error of at most 0.001.
Values may be sent and summed in bfloat16 or wider, within the bound.
A program may use at most 128 MiB of HBM per device.

```python
import jax
import jax.numpy as jnp

D = 7168
F = 16384
SUB_BLOCKS = 4
SEQS = 512
N_ROW = 2
N_COL = 4


def block_scale(rng, shape, cuts, least, high):
    def one(dim, shards_of):
        heights = jax.random.uniform(jax.random.fold_in(jax.random.fold_in(rng, 6), dim), (shards_of,), jnp.float32, least / len(cuts), high / len(cuts))
        return jnp.repeat(jnp.exp(heights), shape[dim] // shards_of).reshape((-1,) + (1,) * (len(shape) - dim - 1))

    loudness = one(*cuts[0])
    for cut in cuts[1:]:
        loudness = loudness * one(*cut)
    return loudness


def centred(key, extent, width, reach, split=(), dtype=jnp.bfloat16):
    drawn = width * jax.random.normal(key, extent, jnp.float32)
    if split:
        drawn = drawn * block_scale(key, extent, split, -0.22, 0.18)
    return jnp.clip(drawn, -reach, reach).astype(dtype)


def setup_inputs(seed: int = 0) -> dict:
    arg_keys = jax.random.split(jax.random.key(seed), 4)
    hidden = centred(arg_keys[0], (SEQS, D), 1.0, 6.0, ((0, 4),))
    train_weight = centred(arg_keys[1], (D, F), D ** -0.5, 0.0625, ((0, 8), (1, 4)))
    shard_order = jax.vmap(lambda own: jax.random.permutation(own, N_ROW))(jax.random.split(arg_keys[2], N_COL * SUB_BLOCKS)).reshape((N_COL, SUB_BLOCKS, N_ROW)).astype(jnp.int32)
    return dict(hidden=hidden, train_weight=train_weight, shard_order=shard_order)


def reference(hidden, train_weight, shard_order):
    block_cols = F // (N_ROW * N_COL)
    sub_cols = block_cols // SUB_BLOCKS
    blocks = train_weight.reshape(D, N_COL, N_ROW, SUB_BLOCKS, sub_cols)
    order = shard_order.astype(jnp.int32)
    pieces = []
    for index in range(SUB_BLOCKS):
        subset = blocks[:, :, :, index, :]
        picks = jnp.broadcast_to(order[:, index, :][None, :, :, None], subset.shape)
        pieces.append(jnp.take_along_axis(subset, picks, axis=2))
    served = jnp.stack(pieces, axis=3).reshape(D, F)
    projected = jnp.dot(hidden, served, preferred_element_type=jnp.float32)
    return served, projected
```

```python
import functools

import jax
import jax.numpy as jnp
from jax import lax
from jax.experimental import pallas as pl
from jax.experimental.pallas import tpu as pltpu
from jax.sharding import PartitionSpec as P

MESH = pl.DeviceIdType.MESH
LANES = 128
MIB = 1024 * 1024
LATE_CHUNKS = (0, 0)


def ordered_pieces(tile, shard_order):
    _, sub_count, row_count = shard_order.shape
    rows_tile, cols_tile = tile.shape
    piece_cols = cols_tile // row_count
    sub_cols = piece_cols // sub_count
    my_order = lax.dynamic_index_in_dim(shard_order, lax.axis_index("col"), 0, keepdims=False)
    blocks = tile.reshape(rows_tile, row_count, sub_count, sub_cols)
    pieces = []
    for s in range(row_count):
        piece = blocks[:, 0]
        for j in range(1, row_count):
            piece = jnp.where((my_order[:, s] == j)[None, :, None], blocks[:, j], piece)
        pieces.append(piece.reshape(rows_tile, piece_cols))
    return jnp.concatenate(pieces, axis=1)


def late_start(chunks, late):
    return chunks - jnp.where(lax.rem(lax.axis_index("col"), 2) == 0, late[0], late[1])


def row_tiles(cols):
    return 256 if cols % 256 == 0 else LANES


def handoff_kernel(
    n_row, n_rep, chunks, late, reorder,
    order_ref, tile_ref, hidden_hbm, full_ref, projected_ref,
    raw_ref, away_ref, hidden_ref, raw_sem, hidden_sem, y_send, y_recv, z_recv, up_send, down_send,
):
    r, c, z = lax.axis_index("row"), lax.axis_index("col"), lax.axis_index("rep")
    rows_tile, cols_tile = tile_ref.shape
    cols = cols_tile // n_row
    rows = rows_tile // chunks
    has_up, has_down = z < n_rep - 1, z > 0
    above = (r, c, jnp.minimum(z + 1, n_rep - 1))
    below = (r, c, jnp.maximum(z - 1, 0))
    per_level = n_row * chunks
    mine = z * n_row + r
    kept = (n_row - 1) * chunks + late_start(chunks, late)

    barrier = pltpu.get_barrier_semaphore()
    for t in range(1, n_row):
        pl.semaphore_signal(barrier, inc=1, device_id=(lax.rem(r + t, n_row), c, z), device_id_type=MESH)

    @pl.when(has_up)
    def _():
        pl.semaphore_signal(barrier, inc=1, device_id=above, device_id_type=MESH)

    @pl.when(has_down)
    def _():
        pl.semaphore_signal(barrier, inc=1, device_id=below, device_id_type=MESH)

    def chunk_of(ref, block, q):
        return ref.at[pl.ds(pl.multiple_of(block * rows_tile + q * rows, 8), rows)]

    def staged(q):
        return pltpu.make_async_copy(chunk_of(tile_ref, 0, q), chunk_of(raw_ref, 0, q), raw_sem.at[q])

    @pl.loop(0, chunks)
    def _(q):
        staged(q).start()

    hidden_copy = pltpu.make_async_copy(hidden_hbm, hidden_ref, hidden_sem)
    hidden_copy.start()

    sub_count = order_ref.shape[2]
    sub_cols = cols // sub_count
    step = 16 if rows % 16 == 0 else 8

    def arrange(q):
        staged(q).wait()

        @pl.loop(0, rows // step)
        def _(i):
            at = pl.ds(pl.multiple_of(q * rows + i * step, step), step)
            to = pl.ds(pl.multiple_of(mine * rows_tile + q * rows + i * step, step), step)

            def place(t, span, piece):
                if t == 0:
                    full_ref[to, span] = piece
                else:
                    away_ref[t - 1, at, span] = piece

            if reorder:
                for k in range(sub_count):
                    blocks = [raw_ref[at, pl.ds(j * cols + k * sub_cols, sub_cols)] for j in range(n_row)]
                    for t in range(n_row):
                        s = lax.rem(r + t, n_row)
                        piece = blocks[0]
                        for j in range(1, n_row):
                            piece = jnp.where(order_ref[c, s, k] == j, blocks[j], piece)
                        place(t, pl.ds(k * sub_cols, sub_cols), piece)
            else:
                for t in range(n_row):
                    s = lax.rem(r + t, n_row)
                    place(t, pl.ds(0, cols), raw_ref[at, pl.ds(pl.multiple_of(s * cols, LANES), cols)])

    def along_row(t, q, outward):
        peer = lax.rem(r + t, n_row)
        source = lax.rem(r - t + n_row, n_row)
        return pltpu.make_async_remote_copy(
            src_ref=chunk_of(away_ref.at[t - 1], 0, q),
            dst_ref=chunk_of(full_ref, z * n_row + (r if outward else source), q),
            send_sem=y_send.at[t * chunks + q],
            recv_sem=y_recv.at[t * chunks + q],
            device_id=(peer, c, z),
            device_id_type=MESH,
        )

    def along_rep(block, q, sems, target):
        return pltpu.make_async_remote_copy(
            src_ref=chunk_of(full_ref, block, q),
            dst_ref=chunk_of(full_ref, block, q),
            send_sem=sems.at[block * chunks + q],
            recv_sem=z_recv.at[block * chunks + q],
            device_id=target,
            device_id_type=MESH,
        )

    def forward(block, q):
        @pl.when(has_up)
        def _():
            along_rep(block, q, up_send, above).start()

        @pl.when(has_down)
        def _():
            along_rep(block, q, down_send, below).start()

    by_chunk = rows % LANES == 0
    tile = row_tiles(cols)

    def multiply(first, depth, fresh):
        within = pl.ds(first, depth)

        @pl.loop(0, cols // tile)
        def _(n):
            at = pl.ds(pl.multiple_of(n * tile, tile), tile)
            term = jnp.dot(hidden_ref[:, within], full_ref[within, at], preferred_element_type=jnp.float32)
            projected_ref[:, at] = term if fresh else projected_ref[:, at] + term

    def consume(block, q):
        if by_chunk:
            multiply(pl.multiple_of(block * rows_tile + q * rows, LANES), rows, False)

    def send_own(q):
        forward(mine, q)
        for t in range(1, n_row):
            along_row(t, q, True).start()

    arrange(0)
    pl.semaphore_wait(barrier, n_row - 1 + has_up.astype(jnp.int32) + has_down.astype(jnp.int32))

    @pl.loop(1, chunks)
    def _(q):
        arrange(q)
        send_own(q - 1)

    send_own(chunks - 1)

    if by_chunk:
        projected_ref[...] = jnp.zeros_like(projected_ref)
    hidden_copy.wait()

    @pl.loop(0, chunks)
    def _(q):
        consume(mine, q)

    for t in range(1, n_row):

        @pl.loop(0, chunks)
        def _(q):
            along_row(t, q, False).wait_recv()
            block = z * n_row + lax.rem(r - t + n_row, n_row)
            forward(block, q)
            consume(block, q)

    def block_of(level, i):
        return level * n_row + lax.rem(r - i // chunks + n_row, n_row), lax.rem(i, chunks)

    def arrived(level, i, sems, target, onward):
        block, q = block_of(level, i)
        copy = along_rep(block, q, sems, target)
        copy.wait_recv()

        @pl.when(onward)
        def _():
            copy.start()

        consume(block, q)

    @pl.loop(1, n_rep)
    def _(d):
        @pl.loop(0, per_level)
        def _(i):
            @pl.when(z - d >= 0)
            def _():
                @pl.when((d < n_rep - 1) | (i < kept))
                def _():
                    arrived(z - d, i, up_send, above, has_up & ((z - d > 0) | (z + 1 < n_rep - 1) | (i < kept)))

            @pl.when(z + d < n_rep)
            def _():
                @pl.when((d < n_rep - 1) | (i < kept))
                def _():
                    arrived(z + d, i, down_send, below, has_down & ((z + d < n_rep - 1) | (z > 1) | (i < kept)))

    if not by_chunk:
        multiply(0, full_ref.shape[0], True)

    @pl.loop(0, chunks)
    def _(q):
        for t in range(1, n_row):
            along_row(t, q, True).wait_send()

    def drain(level, sent, sems, target):
        @pl.loop(0, sent)
        def _(i):
            block, q = block_of(level, i)
            along_rep(block, q, sems, target).wait_send()

    @pl.when(has_up)
    def _():
        @pl.loop(0, z + 1)
        def _(level):
            drain(level, jnp.where((level == 0) & (z + 1 == n_rep - 1), kept, per_level), up_send, above)

    @pl.when(has_down)
    def _():
        @pl.loop(z, n_rep)
        def _(level):
            drain(level, jnp.where((level == n_rep - 1) & (z == 1), kept, per_level), down_send, below)


def vmem():
    return pl.BlockSpec(memory_space=pltpu.VMEM)


def in_hbm(x):
    return pltpu.with_memory_space_constraint(x, pltpu.HBM)


def hbm():
    return pl.BlockSpec(memory_space=pltpu.HBM)


def handed_off(hidden, tile, shard_order, chunks, late, reorder):
    n_row, n_rep = lax.axis_size("row"), lax.axis_size("rep")
    rows_tile, cols_tile = tile.shape
    cols = cols_tile // n_row
    every = n_rep * n_row * chunks
    dma = pltpu.SemaphoreType.DMA
    height = n_rep * n_row * rows_tile
    return pl.pallas_call(
        functools.partial(handoff_kernel, n_row, n_rep, chunks, late, reorder),
        out_shape=(
            pltpu.VMEM((height, cols), tile.dtype),
            pltpu.VMEM((hidden.shape[0], cols), jnp.float32),
        ),
        in_specs=[pl.BlockSpec(memory_space=pltpu.SMEM), hbm(), hbm()],
        out_specs=(vmem(), vmem()),
        scratch_shapes=[
            pltpu.VMEM((rows_tile, cols_tile), tile.dtype),
            pltpu.VMEM((n_row - 1, rows_tile, cols), tile.dtype),
            pltpu.VMEM(hidden.shape, hidden.dtype),
            dma((chunks,)),
            dma,
            dma((n_row * chunks,)),
            dma((n_row * chunks,)),
            dma((every,)),
            dma((every,)),
            dma((every,)),
        ],
        compiler_params=pltpu.CompilerParams(
            collective_id=0, has_side_effects=True, vmem_limit_bytes=14 * MIB
        ),
    )(jnp.swapaxes(shard_order, 1, 2), in_hbm(tile), in_hbm(hidden))


def store_kernel(landed_ref, served_ref, sem):
    parts = sem.shape[0] - 1
    rows = served_ref.shape[0] // parts
    copies = [
        pltpu.make_async_copy(
            landed_ref.at[pl.ds(i * rows, rows)], served_ref.at[pl.ds(i * rows, rows)], sem.at[i]
        )
        for i in range(parts)
    ]
    for copy in copies:
        copy.start()
    for copy in copies:
        copy.wait()


def stored(landed, summed):
    return pl.pallas_call(
        store_kernel,
        out_shape=jax.ShapeDtypeStruct(landed.shape, landed.dtype),
        in_specs=[pl.BlockSpec(memory_space=pl.ANY)],
        out_specs=pl.BlockSpec(memory_space=pl.ANY),
        scratch_shapes=[pltpu.SemaphoreType.DMA((9,))],
        compiler_params=pltpu.CompilerParams(vmem_limit_bytes=MIB),
    )(landed), summed


def shards(hidden, train_weight, shard_order):
    _, sub_count, n_row = shard_order.shape
    rows_tile, cols_tile = train_weight.shape
    chunks = rows_tile // LANES if rows_tile % LANES == 0 else 1
    late = LATE_CHUNKS if chunks > max(LATE_CHUNKS) else (0, 0)
    reorder = (cols_tile // (n_row * sub_count)) % LANES == 0
    tile = train_weight if reorder else ordered_pieces(train_weight, shard_order)
    landed, summed = handed_off(hidden, tile, shard_order, chunks, late, reorder)
    return stored(landed, summed)


def solution(mesh):
    placed = (P("rep", None), P(("rep", "row"), "col"), P())
    return jax.shard_map(
        shards,
        mesh=mesh,
        in_specs=placed,
        out_specs=(P(None, ("col", "row")), P("rep", ("col", "row"))),
        check_vma=False,
    )
```

```python
import functools

import jax
import jax.numpy as jnp
from jax import lax
from jax.experimental import pallas as pl
from jax.experimental.pallas import tpu as pltpu
from jax.sharding import PartitionSpec as P

MESH = pl.DeviceIdType.MESH
LANES = 128
MIB = 1024 * 1024
LATE_CHUNKS = (6, 3)


def ordered_pieces(tile, shard_order):
    _, sub_count, row_count = shard_order.shape
    rows_tile, cols_tile = tile.shape
    piece_cols = cols_tile // row_count
    sub_cols = piece_cols // sub_count
    my_order = lax.dynamic_index_in_dim(shard_order, lax.axis_index("col"), 0, keepdims=False)
    blocks = tile.reshape(rows_tile, row_count, sub_count, sub_cols)
    pieces = []
    for s in range(row_count):
        piece = blocks[:, 0]
        for j in range(1, row_count):
            piece = jnp.where((my_order[:, s] == j)[None, :, None], blocks[:, j], piece)
        pieces.append(piece.reshape(rows_tile, piece_cols))
    return jnp.concatenate(pieces, axis=1)


def late_start(chunks, late):
    return chunks - jnp.where(lax.rem(lax.axis_index("col"), 2) == 0, late[0], late[1])


def row_tiles(cols):
    return 256 if cols % 256 == 0 else LANES


def handoff_kernel(
    n_row, n_rep, chunks, late, reorder,
    order_ref, tile_ref, hidden_hbm, full_ref, projected_ref, keep_ref,
    raw_ref, away_ref, hidden_ref, raw_sem, hidden_sem, y_send, y_recv, z_recv, up_send, down_send,
):
    r, c, z = lax.axis_index("row"), lax.axis_index("col"), lax.axis_index("rep")
    rows_tile, cols_tile = tile_ref.shape
    cols = cols_tile // n_row
    rows = rows_tile // chunks
    has_up, has_down = z < n_rep - 1, z > 0
    above = (r, c, jnp.minimum(z + 1, n_rep - 1))
    below = (r, c, jnp.maximum(z - 1, 0))
    per_level = n_row * chunks
    mine = z * n_row + r
    kept = (n_row - 1) * chunks + late_start(chunks, late)

    barrier = pltpu.get_barrier_semaphore()
    for t in range(1, n_row):
        pl.semaphore_signal(barrier, inc=1, device_id=(lax.rem(r + t, n_row), c, z), device_id_type=MESH)

    @pl.when(has_up)
    def _():
        pl.semaphore_signal(barrier, inc=1, device_id=above, device_id_type=MESH)

    @pl.when(has_down)
    def _():
        pl.semaphore_signal(barrier, inc=1, device_id=below, device_id_type=MESH)

    def chunk_of(ref, block, q):
        return ref.at[pl.ds(pl.multiple_of(block * rows_tile + q * rows, 8), rows)]

    def staged(q):
        return pltpu.make_async_copy(chunk_of(tile_ref, 0, q), chunk_of(raw_ref, 0, q), raw_sem.at[q])

    @pl.loop(0, chunks)
    def _(q):
        staged(q).start()

    hidden_copy = pltpu.make_async_copy(hidden_hbm, hidden_ref, hidden_sem)
    hidden_copy.start()

    sub_count = order_ref.shape[2]
    sub_cols = cols // sub_count
    step = 16 if rows % 16 == 0 else 8

    def arrange(q):
        staged(q).wait()

        @pl.loop(0, rows // step)
        def _(i):
            at = pl.ds(pl.multiple_of(q * rows + i * step, step), step)
            to = pl.ds(pl.multiple_of(mine * rows_tile + q * rows + i * step, step), step)

            def place(t, span, piece):
                if t == 0:
                    full_ref[to, span] = piece
                else:
                    away_ref[t - 1, at, span] = piece

            if reorder:
                for k in range(sub_count):
                    blocks = [raw_ref[at, pl.ds(j * cols + k * sub_cols, sub_cols)] for j in range(n_row)]
                    for t in range(n_row):
                        s = lax.rem(r + t, n_row)
                        piece = blocks[0]
                        for j in range(1, n_row):
                            piece = jnp.where(order_ref[c, s, k] == j, blocks[j], piece)
                        place(t, pl.ds(k * sub_cols, sub_cols), piece)
            else:
                for t in range(n_row):
                    s = lax.rem(r + t, n_row)
                    place(t, pl.ds(0, cols), raw_ref[at, pl.ds(pl.multiple_of(s * cols, LANES), cols)])

    def along_row(t, q, outward):
        peer = lax.rem(r + t, n_row)
        source = lax.rem(r - t + n_row, n_row)
        return pltpu.make_async_remote_copy(
            src_ref=chunk_of(away_ref.at[t - 1], 0, q),
            dst_ref=chunk_of(full_ref, z * n_row + (r if outward else source), q),
            send_sem=y_send.at[t * chunks + q],
            recv_sem=y_recv.at[t * chunks + q],
            device_id=(peer, c, z),
            device_id_type=MESH,
        )

    def along_rep(block, q, sems, target):
        return pltpu.make_async_remote_copy(
            src_ref=chunk_of(full_ref, block, q),
            dst_ref=chunk_of(full_ref, block, q),
            send_sem=sems.at[block * chunks + q],
            recv_sem=z_recv.at[block * chunks + q],
            device_id=target,
            device_id_type=MESH,
        )

    def forward(block, q):
        @pl.when(has_up)
        def _():
            along_rep(block, q, up_send, above).start()

        @pl.when(has_down)
        def _():
            along_rep(block, q, down_send, below).start()

    by_chunk = rows % LANES == 0
    tile = row_tiles(cols)

    def multiply(first, depth, fresh):
        within = pl.ds(first, depth)

        @pl.loop(0, cols // tile)
        def _(n):
            at = pl.ds(pl.multiple_of(n * tile, tile), tile)
            term = jnp.dot(hidden_ref[:, within], full_ref[within, at], preferred_element_type=jnp.float32)
            projected_ref[:, at] = term if fresh else projected_ref[:, at] + term

    def consume(block, q):
        if by_chunk:
            multiply(pl.multiple_of(block * rows_tile + q * rows, LANES), rows, False)

    def send_own(q):
        forward(mine, q)
        for t in range(1, n_row):
            along_row(t, q, True).start()

    arrange(0)
    pl.semaphore_wait(barrier, n_row - 1 + has_up.astype(jnp.int32) + has_down.astype(jnp.int32))

    @pl.loop(1, chunks)
    def _(q):
        arrange(q)
        send_own(q - 1)

    send_own(chunks - 1)

    if by_chunk:
        projected_ref[...] = jnp.zeros_like(projected_ref)
    hidden_copy.wait()

    @pl.loop(0, chunks)
    def _(q):
        consume(mine, q)

    for t in range(1, n_row):

        @pl.loop(0, chunks)
        def _(q):
            along_row(t, q, False).wait_recv()
            block = z * n_row + lax.rem(r - t + n_row, n_row)
            forward(block, q)
            consume(block, q)

    def block_of(level, i):
        return level * n_row + lax.rem(r - i // chunks + n_row, n_row), lax.rem(i, chunks)

    def arrived(d, level, i, sems, target, onward):
        block, q = block_of(level, i)
        copy = along_rep(block, q, sems, target)
        copy.wait_recv()
        deferred = (d == n_rep - 2) & (i >= kept)

        @pl.when(onward & jnp.logical_not(deferred))
        def _():
            copy.start()

        consume(block, q)
        if max(late):

            @pl.when(onward & deferred)
            def _():
                slot = q - (chunks - max(late))
                keep_ref[pl.ds(pl.multiple_of(slot * rows, LANES), rows), :] = full_ref[
                    pl.ds(pl.multiple_of(block * rows_tile + q * rows, LANES), rows), :
                ]

    @pl.loop(1, n_rep)
    def _(d):
        @pl.loop(0, per_level)
        def _(i):
            @pl.when(z - d >= 0)
            def _():
                @pl.when((d < n_rep - 1) | (i < kept))
                def _():
                    arrived(d, z - d, i, up_send, above, has_up)

            @pl.when(z + d < n_rep)
            def _():
                @pl.when((d < n_rep - 1) | (i < kept))
                def _():
                    arrived(d, z + d, i, down_send, below, has_down)

    if not by_chunk:
        multiply(0, full_ref.shape[0], True)

    @pl.loop(0, chunks)
    def _(q):
        for t in range(1, n_row):
            along_row(t, q, True).wait_send()

    def drain(level, sent, sems, target):
        @pl.loop(0, sent)
        def _(i):
            block, q = block_of(level, i)
            along_rep(block, q, sems, target).wait_send()

    @pl.when(has_up)
    def _():
        @pl.loop(0, z + 1)
        def _(level):
            drain(level, jnp.where((level == 0) & (z + 1 == n_rep - 1), kept, per_level), up_send, above)

    @pl.when(has_down)
    def _():
        @pl.loop(z, n_rep)
        def _(level):
            drain(level, jnp.where((level == n_rep - 1) & (z == 1), kept, per_level), down_send, below)


def vmem():
    return pl.BlockSpec(memory_space=pltpu.VMEM)


def in_hbm(x):
    return pltpu.with_memory_space_constraint(x, pltpu.HBM)


def hbm():
    return pl.BlockSpec(memory_space=pltpu.HBM)


def handed_off(hidden, tile, shard_order, chunks, late, reorder):
    n_row, n_rep = lax.axis_size("row"), lax.axis_size("rep")
    rows_tile, cols_tile = tile.shape
    cols = cols_tile // n_row
    every = n_rep * n_row * chunks
    dma = pltpu.SemaphoreType.DMA
    height = n_rep * n_row * rows_tile
    return pl.pallas_call(
        functools.partial(handoff_kernel, n_row, n_rep, chunks, late, reorder),
        out_shape=(
            pltpu.VMEM((height, cols), tile.dtype),
            pltpu.VMEM((hidden.shape[0], cols), jnp.float32),
            pltpu.VMEM((max(8, max(late) * (rows_tile // chunks)), cols), tile.dtype),
        ),
        in_specs=[pl.BlockSpec(memory_space=pltpu.SMEM), hbm(), hbm()],
        out_specs=(vmem(),) * 3,
        scratch_shapes=[
            pltpu.VMEM((rows_tile, cols_tile), tile.dtype),
            pltpu.VMEM((n_row - 1, rows_tile, cols), tile.dtype),
            pltpu.VMEM(hidden.shape, hidden.dtype),
            dma((chunks,)),
            dma,
            dma((n_row * chunks,)),
            dma((n_row * chunks,)),
            dma((every,)),
            dma((every,)),
            dma((every,)),
        ],
        compiler_params=pltpu.CompilerParams(
            collective_id=0, has_side_effects=True, vmem_limit_bytes=14 * MIB
        ),
    )(jnp.swapaxes(shard_order, 1, 2), in_hbm(tile), in_hbm(hidden))


def store_kernel(landed_ref, served_ref, sem):
    parts = sem.shape[0]
    rows = served_ref.shape[0] // parts
    copies = [
        pltpu.make_async_copy(
            landed_ref.at[pl.ds(i * rows, rows)], served_ref.at[pl.ds(i * rows, rows)], sem.at[i]
        )
        for i in range(parts)
    ]
    for copy in copies:
        copy.start()
    for copy in copies:
        copy.wait()


def stored(landed):
    return pl.pallas_call(
        store_kernel,
        out_shape=jax.ShapeDtypeStruct(landed.shape, landed.dtype),
        in_specs=[pl.BlockSpec(memory_space=pl.ANY)],
        out_specs=pl.BlockSpec(memory_space=pl.ANY),
        scratch_shapes=[pltpu.SemaphoreType.DMA((8,))],
        compiler_params=pltpu.CompilerParams(vmem_limit_bytes=MIB),
    )(landed)


def late_kernel(
    n_row, n_rep, chunks, late,
    keep_ref, partial_ref, hidden_hbm, _, late_ref, summed_ref,
    hidden_ref, hidden_sem, send_sem, recv_sem,
):
    r, c, z = lax.axis_index("row"), lax.axis_index("col"), lax.axis_index("rep")
    slots = max(late)
    rows, cols = late_ref.shape[0] // slots, late_ref.shape[1]
    first = late_start(chunks, late)
    other = lax.rem(r + 1, n_row)
    lowest, highest = other, (n_rep - 1) * n_row + other
    gives_up, gives_down = z == n_rep - 2, z == 1
    takes_below, takes_above = z == n_rep - 1, z == 0
    above = (r, c, jnp.minimum(z + 1, n_rep - 1))
    below = (r, c, jnp.maximum(z - 1, 0))

    barrier = pltpu.get_barrier_semaphore()

    @pl.when(gives_up | takes_above)
    def _():
        pl.semaphore_signal(barrier, inc=1, device_id=above, device_id_type=MESH)

    @pl.when(gives_down | takes_below)
    def _():
        pl.semaphore_signal(barrier, inc=1, device_id=below, device_id_type=MESH)

    pl.semaphore_wait(barrier, (gives_up | takes_above).astype(jnp.int32) + (gives_down | takes_below).astype(jnp.int32))

    def moved(q, target):
        slot = q - (chunks - slots)
        return pltpu.make_async_remote_copy(
            src_ref=keep_ref.at[pl.ds(pl.multiple_of(slot * rows, LANES), rows)],
            dst_ref=late_ref.at[pl.ds(pl.multiple_of(slot * rows, LANES), rows)],
            send_sem=send_sem.at[slot],
            recv_sem=recv_sem.at[slot],
            device_id=target,
            device_id_type=MESH,
        )

    @pl.when(gives_up)
    def _():
        @pl.loop(first, chunks)
        def _(q):
            moved(q, above).start()

    @pl.when(gives_down)
    def _():
        @pl.loop(first, chunks)
        def _(q):
            moved(q, below).start()

    summed_ref[...] = partial_ref[...]
    tile = row_tiles(cols)

    def take(block, target):
        hidden_copy = pltpu.make_async_copy(
            hidden_hbm.at[:, pl.ds(pl.multiple_of((block * chunks + chunks - slots) * rows, LANES), slots * rows)],
            hidden_ref,
            hidden_sem,
        )
        hidden_copy.start()
        hidden_copy.wait()

        @pl.loop(first, chunks)
        def _(q):
            moved(q, target).wait_recv()
            within = pl.ds(pl.multiple_of((q - (chunks - slots)) * rows, LANES), rows)
            for n in range(cols // tile):
                at = pl.ds(n * tile, tile)
                summed_ref[:, at] += jnp.dot(
                    hidden_ref[:, within], late_ref[within, at], preferred_element_type=jnp.float32
                )

    @pl.when(takes_below)
    def _():
        take(lowest, below)

    @pl.when(takes_above)
    def _():
        take(highest, above)

    @pl.when(gives_up)
    def _():
        @pl.loop(first, chunks)
        def _(q):
            moved(q, above).wait_send()

    @pl.when(gives_down)
    def _():
        @pl.loop(first, chunks)
        def _(q):
            moved(q, below).wait_send()


def late_handoff(keep, partial, hidden, token, chunks, late):
    n_row, n_rep = lax.axis_size("row"), lax.axis_size("rep")
    slots = max(late)
    rows = keep.shape[0] // slots
    dma = pltpu.SemaphoreType.DMA
    return pl.pallas_call(
        functools.partial(late_kernel, n_row, n_rep, chunks, late),
        out_shape=(
            pltpu.VMEM(keep.shape, keep.dtype),
            pltpu.VMEM(partial.shape, partial.dtype),
        ),
        in_specs=[vmem(), vmem(), hbm(), hbm()],
        out_specs=(vmem(), vmem()),
        scratch_shapes=[
            pltpu.VMEM((hidden.shape[0], slots * rows), hidden.dtype),
            dma,
            dma((slots,)),
            dma((slots,)),
        ],
        cost_estimate=pl.CostEstimate(flops=10**11, bytes_accessed=10**6, transcendentals=0),
        compiler_params=pltpu.CompilerParams(
            collective_id=1, has_side_effects=True, vmem_limit_bytes=2 * MIB
        ),
    )(keep, partial, in_hbm(hidden), in_hbm(token))


def finish_kernel(n_row, n_rep, chunks, late, early_ref, late_ref, summed_ref, served_ref, projected_ref, sem, projected_sem):
    r, z = lax.axis_index("row"), lax.axis_index("rep")
    rows_tile = served_ref.shape[0] // (n_row * n_rep)
    rows = rows_tile // chunks
    slots = late_ref.shape[0] // rows
    first = late_start(chunks, late)
    block = jnp.where(z == 0, n_rep - 1, 0) * n_row + lax.rem(r + 1, n_row)
    takes = (z == 0) | (z == n_rep - 1)

    def stored(q):
        slot = q - (chunks - slots)
        return pltpu.make_async_copy(
            late_ref.at[pl.ds(pl.multiple_of(slot * rows, LANES), rows)],
            served_ref.at[pl.ds(pl.multiple_of(block * rows_tile + q * rows, LANES), rows)],
            sem.at[slot],
        )

    projected_copy = pltpu.make_async_copy(summed_ref, projected_ref, projected_sem)
    projected_copy.start()

    @pl.when(takes)
    def _():
        @pl.loop(first, chunks)
        def _(q):
            stored(q).start()

        @pl.loop(first, chunks)
        def _(q):
            stored(q).wait()

    projected_copy.wait()


def finished(early, landed, summed, chunks, late):
    n_row, n_rep = lax.axis_size("row"), lax.axis_size("rep")
    dma = pltpu.SemaphoreType.DMA
    return pl.pallas_call(
        functools.partial(finish_kernel, n_row, n_rep, chunks, late),
        out_shape=(
            jax.ShapeDtypeStruct(early.shape, early.dtype),
            jax.ShapeDtypeStruct(summed.shape, summed.dtype),
        ),
        in_specs=[pl.BlockSpec(memory_space=pl.ANY), vmem(), vmem()],
        out_specs=(pl.BlockSpec(memory_space=pl.ANY),) * 2,
        scratch_shapes=[dma((max(late),)), dma],
        input_output_aliases={0: 0},
        compiler_params=pltpu.CompilerParams(vmem_limit_bytes=MIB),
    )(early, landed, summed)


def shards(hidden, train_weight, shard_order):
    _, sub_count, n_row = shard_order.shape
    rows_tile, cols_tile = train_weight.shape
    chunks = rows_tile // LANES if rows_tile % LANES == 0 else 1
    late = LATE_CHUNKS if chunks > max(LATE_CHUNKS) and lax.axis_size("rep") > 2 else (0, 0)
    reorder = (cols_tile // (n_row * sub_count)) % LANES == 0
    tile = train_weight if reorder else ordered_pieces(train_weight, shard_order)
    landed, summed, keep = handed_off(hidden, tile, shard_order, chunks, late, reorder)
    served = stored(landed)
    if max(late) == 0:
        return served, summed
    tail, total = late_handoff(keep, summed, hidden, served, chunks, late)
    return finished(served, tail, total, chunks, late)


def solution(mesh):
    placed = (P("rep", None), P(("rep", "row"), "col"), P())
    return jax.shard_map(
        shards,
        mesh=mesh,
        in_specs=placed,
        out_specs=(P(None, ("col", "row")), P("rep", ("col", "row"))),
        check_vma=False,
    )
```

```python
import functools

import jax
import jax.numpy as jnp
from jax import lax
from jax.experimental import pallas as pl
from jax.experimental.pallas import tpu as pltpu
from jax.sharding import PartitionSpec as P

MESH = pl.DeviceIdType.MESH
LANES = 128
MIB = 1024 * 1024
LATE_CHUNKS = (5, 1)


def ordered_pieces(tile, shard_order):
    _, sub_count, row_count = shard_order.shape
    rows_tile, cols_tile = tile.shape
    piece_cols = cols_tile // row_count
    sub_cols = piece_cols // sub_count
    my_order = lax.dynamic_index_in_dim(shard_order, lax.axis_index("col"), 0, keepdims=False)
    blocks = tile.reshape(rows_tile, row_count, sub_count, sub_cols)
    pieces = []
    for s in range(row_count):
        piece = blocks[:, 0]
        for j in range(1, row_count):
            piece = jnp.where((my_order[:, s] == j)[None, :, None], blocks[:, j], piece)
        pieces.append(piece.reshape(rows_tile, piece_cols))
    return jnp.concatenate(pieces, axis=1)


def late_start(chunks, late):
    return chunks - jnp.where(lax.rem(lax.axis_index("col"), 2) == 0, late[0], late[1])


def row_tiles(cols):
    return 256 if cols % 256 == 0 else LANES


def handoff_kernel(
    n_row, n_rep, chunks, late, reorder,
    order_hbm, tile_ref, hidden_hbm, full_ref, projected_ref, keep_ref,
    order_ref, raw_ref, away_ref, hidden_ref, order_sem, raw_sem, hidden_sem, y_send, y_recv, z_recv, up_send, down_send,
):
    r, c, z = lax.axis_index("row"), lax.axis_index("col"), lax.axis_index("rep")
    rows_tile, cols_tile = tile_ref.shape
    cols = cols_tile // n_row
    rows = rows_tile // chunks
    has_up, has_down = z < n_rep - 1, z > 0
    above = (r, c, jnp.minimum(z + 1, n_rep - 1))
    below = (r, c, jnp.maximum(z - 1, 0))
    per_level = n_row * chunks
    mine = z * n_row + r
    kept = (n_row - 1) * chunks + late_start(chunks, late)

    barrier = pltpu.get_barrier_semaphore()
    for t in range(1, n_row):
        pl.semaphore_signal(barrier, inc=1, device_id=(lax.rem(r + t, n_row), c, z), device_id_type=MESH)

    @pl.when(has_up)
    def _():
        pl.semaphore_signal(barrier, inc=1, device_id=above, device_id_type=MESH)

    @pl.when(has_down)
    def _():
        pl.semaphore_signal(barrier, inc=1, device_id=below, device_id_type=MESH)

    def chunk_of(ref, block, q):
        return ref.at[pl.ds(pl.multiple_of(block * rows_tile + q * rows, 8), rows)]

    def staged(q):
        return pltpu.make_async_copy(chunk_of(tile_ref, 0, q), chunk_of(raw_ref, 0, q), raw_sem.at[q])

    order_copy = pltpu.make_async_copy(order_hbm, order_ref, order_sem)
    hidden_copy = pltpu.make_async_copy(hidden_hbm, hidden_ref, hidden_sem)
    order_copy.start()
    staged(0).start()

    sub_count = order_ref.shape[2]
    sub_cols = cols // sub_count
    step = 16 if rows % 16 == 0 else 8

    def arrange(q):
        staged(q).wait()

        @pl.loop(0, rows // step)
        def _(i):
            at = pl.ds(pl.multiple_of(q * rows + i * step, step), step)
            to = pl.ds(pl.multiple_of(mine * rows_tile + q * rows + i * step, step), step)

            def place(t, span, piece):
                if t == 0:
                    full_ref[to, span] = piece
                else:
                    away_ref[t - 1, at, span] = piece

            if reorder:
                for k in range(sub_count):
                    blocks = [raw_ref[at, pl.ds(j * cols + k * sub_cols, sub_cols)] for j in range(n_row)]
                    for t in range(n_row):
                        s = lax.rem(r + t, n_row)
                        piece = blocks[0]
                        for j in range(1, n_row):
                            piece = jnp.where(order_ref[c, s, k] == j, blocks[j], piece)
                        place(t, pl.ds(k * sub_cols, sub_cols), piece)
            else:
                for t in range(n_row):
                    s = lax.rem(r + t, n_row)
                    place(t, pl.ds(0, cols), raw_ref[at, pl.ds(pl.multiple_of(s * cols, LANES), cols)])

    def along_row(t, q, outward):
        peer = lax.rem(r + t, n_row)
        source = lax.rem(r - t + n_row, n_row)
        return pltpu.make_async_remote_copy(
            src_ref=chunk_of(away_ref.at[t - 1], 0, q),
            dst_ref=chunk_of(full_ref, z * n_row + (r if outward else source), q),
            send_sem=y_send.at[t * chunks + q],
            recv_sem=y_recv.at[t * chunks + q],
            device_id=(peer, c, z),
            device_id_type=MESH,
        )

    def along_rep(block, q, sems, target):
        return pltpu.make_async_remote_copy(
            src_ref=chunk_of(full_ref, block, q),
            dst_ref=chunk_of(full_ref, block, q),
            send_sem=sems.at[block * chunks + q],
            recv_sem=z_recv.at[block * chunks + q],
            device_id=target,
            device_id_type=MESH,
        )

    def forward(block, q):
        @pl.when(has_up)
        def _():
            along_rep(block, q, up_send, above).start()

        @pl.when(has_down)
        def _():
            along_rep(block, q, down_send, below).start()

    by_chunk = rows % LANES == 0
    tile = row_tiles(cols)

    def multiply(first, depth, fresh):
        within = pl.ds(first, depth)

        @pl.loop(0, cols // tile)
        def _(n):
            at = pl.ds(pl.multiple_of(n * tile, tile), tile)
            term = jnp.dot(hidden_ref[:, within], full_ref[within, at], preferred_element_type=jnp.float32)
            projected_ref[:, at] = term if fresh else projected_ref[:, at] + term

    def consume(block, q):
        if by_chunk:
            multiply(pl.multiple_of(block * rows_tile + q * rows, LANES), rows, False)

    def send_own(q):
        forward(mine, q)
        for t in range(1, n_row):
            along_row(t, q, True).start()

    order_copy.wait()
    arrange(0)

    @pl.loop(1, chunks)
    def _(q):
        staged(q).start()

    hidden_copy.start()
    pl.semaphore_wait(barrier, n_row - 1 + has_up.astype(jnp.int32) + has_down.astype(jnp.int32))
    send_own(0)

    @pl.loop(1, chunks)
    def _(q):
        arrange(q)

        @pl.when(q > 1)
        def _():
            send_own(q - 1)

    if chunks > 1:
        send_own(chunks - 1)

    if by_chunk:
        projected_ref[...] = jnp.zeros_like(projected_ref)
    hidden_copy.wait()

    @pl.loop(0, chunks)
    def _(q):
        consume(mine, q)

    for t in range(1, n_row):

        @pl.loop(0, chunks)
        def _(q):
            along_row(t, q, False).wait_recv()
            block = z * n_row + lax.rem(r - t + n_row, n_row)
            forward(block, q)
            consume(block, q)

    def block_of(level, i):
        return level * n_row + lax.rem(r - i // chunks + n_row, n_row), lax.rem(i, chunks)

    def arrived(d, level, i, sems, target, onward):
        block, q = block_of(level, i)
        copy = along_rep(block, q, sems, target)
        copy.wait_recv()
        deferred = (d == n_rep - 2) & (i >= kept)

        @pl.when(onward & jnp.logical_not(deferred))
        def _():
            copy.start()

        consume(block, q)
        if max(late):

            @pl.when(onward & deferred)
            def _():
                slot = q - (chunks - max(late))
                keep_ref[pl.ds(pl.multiple_of(slot * rows, LANES), rows), :] = full_ref[
                    pl.ds(pl.multiple_of(block * rows_tile + q * rows, LANES), rows), :
                ]

    @pl.loop(1, n_rep)
    def _(d):
        @pl.loop(0, per_level)
        def _(i):
            @pl.when(z - d >= 0)
            def _():
                @pl.when((d < n_rep - 1) | (i < kept))
                def _():
                    arrived(d, z - d, i, up_send, above, has_up)

            @pl.when(z + d < n_rep)
            def _():
                @pl.when((d < n_rep - 1) | (i < kept))
                def _():
                    arrived(d, z + d, i, down_send, below, has_down)

    if not by_chunk:
        multiply(0, full_ref.shape[0], True)

    @pl.loop(0, chunks)
    def _(q):
        for t in range(1, n_row):
            along_row(t, q, True).wait_send()

    def drain(level, sent, sems, target):
        @pl.loop(0, sent)
        def _(i):
            block, q = block_of(level, i)
            along_rep(block, q, sems, target).wait_send()

    @pl.when(has_up)
    def _():
        @pl.loop(0, z + 1)
        def _(level):
            drain(level, jnp.where((level == 0) & (z + 1 == n_rep - 1), kept, per_level), up_send, above)

    @pl.when(has_down)
    def _():
        @pl.loop(z, n_rep)
        def _(level):
            drain(level, jnp.where((level == n_rep - 1) & (z == 1), kept, per_level), down_send, below)


def vmem():
    return pl.BlockSpec(memory_space=pltpu.VMEM)


def in_hbm(x):
    return pltpu.with_memory_space_constraint(x, pltpu.HBM)


def hbm():
    return pl.BlockSpec(memory_space=pltpu.HBM)


def handed_off(hidden, tile, shard_order, chunks, late, reorder):
    n_row, n_rep = lax.axis_size("row"), lax.axis_size("rep")
    rows_tile, cols_tile = tile.shape
    cols = cols_tile // n_row
    every = n_rep * n_row * chunks
    order = jnp.swapaxes(shard_order, 1, 2)
    dma = pltpu.SemaphoreType.DMA
    height = n_rep * n_row * rows_tile
    return pl.pallas_call(
        functools.partial(handoff_kernel, n_row, n_rep, chunks, late, reorder),
        out_shape=(
            pltpu.VMEM((height, cols), tile.dtype),
            pltpu.VMEM((hidden.shape[0], cols), jnp.float32),
            pltpu.VMEM((max(8, max(late) * (rows_tile // chunks)), cols), tile.dtype),
        ),
        in_specs=[hbm(), hbm(), hbm()],
        out_specs=(vmem(),) * 3,
        scratch_shapes=[
            pltpu.SMEM(order.shape, order.dtype),
            pltpu.VMEM((rows_tile, cols_tile), tile.dtype),
            pltpu.VMEM((n_row - 1, rows_tile, cols), tile.dtype),
            pltpu.VMEM(hidden.shape, hidden.dtype),
            dma,
            dma((chunks,)),
            dma,
            dma((n_row * chunks,)),
            dma((n_row * chunks,)),
            dma((every,)),
            dma((every,)),
            dma((every,)),
        ],
        compiler_params=pltpu.CompilerParams(
            collective_id=0, has_side_effects=True, vmem_limit_bytes=14 * MIB
        ),
    )(in_hbm(order), in_hbm(tile), in_hbm(hidden))


def store_kernel(landed_ref, served_ref, sem):
    parts = sem.shape[0]
    rows = served_ref.shape[0] // parts
    copies = [
        pltpu.make_async_copy(
            landed_ref.at[pl.ds(i * rows, rows)], served_ref.at[pl.ds(i * rows, rows)], sem.at[i]
        )
        for i in range(parts)
    ]
    for copy in copies:
        copy.start()
    for copy in copies:
        copy.wait()


def stored(landed):
    return pl.pallas_call(
        store_kernel,
        out_shape=jax.ShapeDtypeStruct(landed.shape, landed.dtype),
        in_specs=[pl.BlockSpec(memory_space=pl.ANY)],
        out_specs=pl.BlockSpec(memory_space=pl.ANY),
        scratch_shapes=[pltpu.SemaphoreType.DMA((8,))],
        compiler_params=pltpu.CompilerParams(vmem_limit_bytes=MIB),
    )(landed)


def late_kernel(
    n_row, n_rep, chunks, late,
    keep_ref, partial_ref, hidden_hbm, _, late_ref, summed_ref,
    hidden_ref, hidden_sem, send_sem, recv_sem,
):
    r, c, z = lax.axis_index("row"), lax.axis_index("col"), lax.axis_index("rep")
    slots = max(late)
    rows, cols = late_ref.shape[0] // slots, late_ref.shape[1]
    first = late_start(chunks, late)
    other = lax.rem(r + 1, n_row)
    lowest, highest = other, (n_rep - 1) * n_row + other
    gives_up, gives_down = z == n_rep - 2, z == 1
    takes_below, takes_above = z == n_rep - 1, z == 0
    above = (r, c, jnp.minimum(z + 1, n_rep - 1))
    below = (r, c, jnp.maximum(z - 1, 0))

    barrier = pltpu.get_barrier_semaphore()

    @pl.when(gives_up | takes_above)
    def _():
        pl.semaphore_signal(barrier, inc=1, device_id=above, device_id_type=MESH)

    @pl.when(gives_down | takes_below)
    def _():
        pl.semaphore_signal(barrier, inc=1, device_id=below, device_id_type=MESH)

    pl.semaphore_wait(barrier, (gives_up | takes_above).astype(jnp.int32) + (gives_down | takes_below).astype(jnp.int32))

    def moved(q, target):
        slot = q - (chunks - slots)
        return pltpu.make_async_remote_copy(
            src_ref=keep_ref.at[pl.ds(pl.multiple_of(slot * rows, LANES), rows)],
            dst_ref=late_ref.at[pl.ds(pl.multiple_of(slot * rows, LANES), rows)],
            send_sem=send_sem.at[slot],
            recv_sem=recv_sem.at[slot],
            device_id=target,
            device_id_type=MESH,
        )

    @pl.when(gives_up)
    def _():
        @pl.loop(first, chunks)
        def _(q):
            moved(q, above).start()

    @pl.when(gives_down)
    def _():
        @pl.loop(first, chunks)
        def _(q):
            moved(q, below).start()

    summed_ref[...] = partial_ref[...]
    tile = row_tiles(cols)

    def take(block, target):
        hidden_copy = pltpu.make_async_copy(
            hidden_hbm.at[:, pl.ds(pl.multiple_of((block * chunks + chunks - slots) * rows, LANES), slots * rows)],
            hidden_ref,
            hidden_sem,
        )
        hidden_copy.start()
        hidden_copy.wait()

        @pl.loop(first, chunks)
        def _(q):
            moved(q, target).wait_recv()
            within = pl.ds(pl.multiple_of((q - (chunks - slots)) * rows, LANES), rows)
            for n in range(cols // tile):
                at = pl.ds(n * tile, tile)
                summed_ref[:, at] += jnp.dot(
                    hidden_ref[:, within], late_ref[within, at], preferred_element_type=jnp.float32
                )

    @pl.when(takes_below)
    def _():
        take(lowest, below)

    @pl.when(takes_above)
    def _():
        take(highest, above)

    @pl.when(gives_up)
    def _():
        @pl.loop(first, chunks)
        def _(q):
            moved(q, above).wait_send()

    @pl.when(gives_down)
    def _():
        @pl.loop(first, chunks)
        def _(q):
            moved(q, below).wait_send()


def late_handoff(keep, partial, hidden, token, chunks, late):
    n_row, n_rep = lax.axis_size("row"), lax.axis_size("rep")
    slots = max(late)
    rows = keep.shape[0] // slots
    dma = pltpu.SemaphoreType.DMA
    return pl.pallas_call(
        functools.partial(late_kernel, n_row, n_rep, chunks, late),
        out_shape=(
            pltpu.VMEM(keep.shape, keep.dtype),
            pltpu.VMEM(partial.shape, partial.dtype),
        ),
        in_specs=[vmem(), vmem(), hbm(), hbm()],
        out_specs=(vmem(), vmem()),
        scratch_shapes=[
            pltpu.VMEM((hidden.shape[0], slots * rows), hidden.dtype),
            dma,
            dma((slots,)),
            dma((slots,)),
        ],
        cost_estimate=pl.CostEstimate(flops=10**11, bytes_accessed=10**6, transcendentals=0),
        compiler_params=pltpu.CompilerParams(
            collective_id=1, has_side_effects=True, vmem_limit_bytes=2 * MIB
        ),
    )(keep, partial, in_hbm(hidden), in_hbm(token))


def finish_kernel(n_row, n_rep, chunks, late, early_ref, late_ref, summed_ref, served_ref, projected_ref, sem, projected_sem):
    r, z = lax.axis_index("row"), lax.axis_index("rep")
    rows_tile = served_ref.shape[0] // (n_row * n_rep)
    rows = rows_tile // chunks
    slots = late_ref.shape[0] // rows
    first = late_start(chunks, late)
    block = jnp.where(z == 0, n_rep - 1, 0) * n_row + lax.rem(r + 1, n_row)
    takes = (z == 0) | (z == n_rep - 1)

    def stored(q):
        slot = q - (chunks - slots)
        return pltpu.make_async_copy(
            late_ref.at[pl.ds(pl.multiple_of(slot * rows, LANES), rows)],
            served_ref.at[pl.ds(pl.multiple_of(block * rows_tile + q * rows, LANES), rows)],
            sem.at[slot],
        )

    projected_copy = pltpu.make_async_copy(summed_ref, projected_ref, projected_sem)
    projected_copy.start()

    @pl.when(takes)
    def _():
        @pl.loop(first, chunks)
        def _(q):
            stored(q).start()

        @pl.loop(first, chunks)
        def _(q):
            stored(q).wait()

    projected_copy.wait()


def finished(early, landed, summed, chunks, late):
    n_row, n_rep = lax.axis_size("row"), lax.axis_size("rep")
    dma = pltpu.SemaphoreType.DMA
    return pl.pallas_call(
        functools.partial(finish_kernel, n_row, n_rep, chunks, late),
        out_shape=(
            jax.ShapeDtypeStruct(early.shape, early.dtype),
            jax.ShapeDtypeStruct(summed.shape, summed.dtype),
        ),
        in_specs=[pl.BlockSpec(memory_space=pl.ANY), vmem(), vmem()],
        out_specs=(pl.BlockSpec(memory_space=pl.ANY),) * 2,
        scratch_shapes=[dma((max(late),)), dma],
        input_output_aliases={0: 0},
        compiler_params=pltpu.CompilerParams(vmem_limit_bytes=MIB),
    )(early, landed, summed)


def shards(hidden, train_weight, shard_order):
    _, sub_count, n_row = shard_order.shape
    rows_tile, cols_tile = train_weight.shape
    chunks = rows_tile // LANES if rows_tile % LANES == 0 else 1
    late = LATE_CHUNKS if chunks > max(LATE_CHUNKS) and lax.axis_size("rep") > 2 else (0, 0)
    reorder = (cols_tile // (n_row * sub_count)) % LANES == 0
    tile = train_weight if reorder else ordered_pieces(train_weight, shard_order)
    landed, summed, keep = handed_off(hidden, tile, shard_order, chunks, late, reorder)
    served = stored(landed)
    if max(late) == 0:
        return served, summed
    tail, total = late_handoff(keep, summed, hidden, served, chunks, late)
    return finished(served, tail, total, chunks, late)


def solution(mesh):
    placed = (P("rep", None), P(("rep", "row"), "col"), P())
    return jax.shard_map(
        shards,
        mesh=mesh,
        in_specs=placed,
        out_specs=(P(None, ("col", "row")), P("rep", ("col", "row"))),
        check_vma=False,
    )
```

```python
import functools

import jax
import jax.numpy as jnp
from jax import lax
from jax.experimental import pallas as pl
from jax.experimental.pallas import tpu as pltpu
from jax.sharding import PartitionSpec as P

MESH = pl.DeviceIdType.MESH
LANES = 128
MIB = 1024 * 1024
LATE_CHUNKS = (1, 6)


def ordered_pieces(tile, shard_order):
    _, sub_count, row_count = shard_order.shape
    rows_tile, cols_tile = tile.shape
    piece_cols = cols_tile // row_count
    sub_cols = piece_cols // sub_count
    my_order = lax.dynamic_index_in_dim(shard_order, lax.axis_index("col"), 0, keepdims=False)
    blocks = tile.reshape(rows_tile, row_count, sub_count, sub_cols)
    pieces = []
    for s in range(row_count):
        piece = blocks[:, 0]
        for j in range(1, row_count):
            piece = jnp.where((my_order[:, s] == j)[None, :, None], blocks[:, j], piece)
        pieces.append(piece.reshape(rows_tile, piece_cols))
    return jnp.concatenate(pieces, axis=1)


def late_start(chunks, late):
    return chunks - jnp.where(lax.rem(lax.axis_index("col"), 2) == 0, late[0], late[1])


def row_tiles(cols):
    return 256 if cols % 256 == 0 else LANES


def handoff_kernel(
    n_row, n_rep, chunks, late, reorder,
    order_hbm, tile_ref, hidden_hbm, full_ref, projected_ref, keep_ref,
    order_ref, raw_ref, away_ref, hidden_ref, order_sem, raw_sem, hidden_sem, y_send, y_recv, z_recv, up_send, down_send,
):
    r, c, z = lax.axis_index("row"), lax.axis_index("col"), lax.axis_index("rep")
    rows_tile, cols_tile = tile_ref.shape
    cols = cols_tile // n_row
    rows = rows_tile // chunks
    has_up, has_down = z < n_rep - 1, z > 0
    above = (r, c, jnp.minimum(z + 1, n_rep - 1))
    below = (r, c, jnp.maximum(z - 1, 0))
    per_level = n_row * chunks
    mine = z * n_row + r
    kept = (n_row - 1) * chunks + late_start(chunks, late)

    barrier = pltpu.get_barrier_semaphore()
    for t in range(1, n_row):
        pl.semaphore_signal(barrier, inc=1, device_id=(lax.rem(r + t, n_row), c, z), device_id_type=MESH)

    @pl.when(has_up)
    def _():
        pl.semaphore_signal(barrier, inc=1, device_id=above, device_id_type=MESH)

    @pl.when(has_down)
    def _():
        pl.semaphore_signal(barrier, inc=1, device_id=below, device_id_type=MESH)

    def chunk_of(ref, block, q):
        return ref.at[pl.ds(pl.multiple_of(block * rows_tile + q * rows, 8), rows)]

    def staged(q):
        return pltpu.make_async_copy(chunk_of(tile_ref, 0, q), chunk_of(raw_ref, 0, q), raw_sem.at[q])

    order_copy = pltpu.make_async_copy(order_hbm, order_ref, order_sem)
    hidden_copy = pltpu.make_async_copy(hidden_hbm, hidden_ref, hidden_sem)
    order_copy.start()
    staged(0).start()

    sub_count = order_ref.shape[2]
    sub_cols = cols // sub_count
    step = 16 if rows % 16 == 0 else 8

    def arrange(q):
        staged(q).wait()

        @pl.loop(0, rows // step)
        def _(i):
            at = pl.ds(pl.multiple_of(q * rows + i * step, step), step)
            to = pl.ds(pl.multiple_of(mine * rows_tile + q * rows + i * step, step), step)

            def place(t, span, piece):
                if t == 0:
                    full_ref[to, span] = piece
                else:
                    away_ref[t - 1, at, span] = piece

            if reorder:
                for k in range(sub_count):
                    blocks = [raw_ref[at, pl.ds(j * cols + k * sub_cols, sub_cols)] for j in range(n_row)]
                    for t in range(n_row):
                        s = lax.rem(r + t, n_row)
                        piece = blocks[0]
                        for j in range(1, n_row):
                            piece = jnp.where(order_ref[c, s, k] == j, blocks[j], piece)
                        place(t, pl.ds(k * sub_cols, sub_cols), piece)
            else:
                for t in range(n_row):
                    s = lax.rem(r + t, n_row)
                    place(t, pl.ds(0, cols), raw_ref[at, pl.ds(pl.multiple_of(s * cols, LANES), cols)])

    def along_row(t, q, outward):
        peer = lax.rem(r + t, n_row)
        source = lax.rem(r - t + n_row, n_row)
        return pltpu.make_async_remote_copy(
            src_ref=chunk_of(away_ref.at[t - 1], 0, q),
            dst_ref=chunk_of(full_ref, z * n_row + (r if outward else source), q),
            send_sem=y_send.at[t * chunks + q],
            recv_sem=y_recv.at[t * chunks + q],
            device_id=(peer, c, z),
            device_id_type=MESH,
        )

    def along_rep(block, q, sems, target):
        return pltpu.make_async_remote_copy(
            src_ref=chunk_of(full_ref, block, q),
            dst_ref=chunk_of(full_ref, block, q),
            send_sem=sems.at[block * chunks + q],
            recv_sem=z_recv.at[block * chunks + q],
            device_id=target,
            device_id_type=MESH,
        )

    def forward(block, q):
        @pl.when(has_up)
        def _():
            along_rep(block, q, up_send, above).start()

        @pl.when(has_down)
        def _():
            along_rep(block, q, down_send, below).start()

    by_chunk = rows % LANES == 0
    tile = row_tiles(cols)

    def multiply(first, depth, fresh):
        within = pl.ds(first, depth)

        @pl.loop(0, cols // tile)
        def _(n):
            at = pl.ds(pl.multiple_of(n * tile, tile), tile)
            term = jnp.dot(hidden_ref[:, within], full_ref[within, at], preferred_element_type=jnp.float32)
            projected_ref[:, at] = term if fresh else projected_ref[:, at] + term

    def consume(block, q):
        if by_chunk:
            multiply(pl.multiple_of(block * rows_tile + q * rows, LANES), rows, False)

    def send_own(q):
        forward(mine, q)
        for t in range(1, n_row):
            along_row(t, q, True).start()

    order_copy.wait()
    arrange(0)

    @pl.loop(1, chunks)
    def _(q):
        staged(q).start()

    hidden_copy.start()
    pl.semaphore_wait(barrier, n_row - 1 + has_up.astype(jnp.int32) + has_down.astype(jnp.int32))
    send_own(0)

    @pl.loop(1, chunks)
    def _(q):
        arrange(q)

        @pl.when(q > 1)
        def _():
            send_own(q - 1)

    if chunks > 1:
        send_own(chunks - 1)

    if by_chunk:
        projected_ref[...] = jnp.zeros_like(projected_ref)
    hidden_copy.wait()

    @pl.loop(0, chunks)
    def _(q):
        consume(mine, q)

    for t in range(1, n_row):

        @pl.loop(0, chunks)
        def _(q):
            along_row(t, q, False).wait_recv()
            block = z * n_row + lax.rem(r - t + n_row, n_row)
            forward(block, q)
            consume(block, q)

    def block_of(level, i):
        return level * n_row + lax.rem(r - i // chunks + n_row, n_row), lax.rem(i, chunks)

    def arrived(d, level, i, sems, target, onward):
        block, q = block_of(level, i)
        copy = along_rep(block, q, sems, target)
        copy.wait_recv()
        deferred = (d == n_rep - 2) & (i >= kept)

        @pl.when(onward & jnp.logical_not(deferred))
        def _():
            copy.start()

        consume(block, q)
        if max(late):

            @pl.when(onward & deferred)
            def _():
                slot = q - (chunks - max(late))
                keep_ref[pl.ds(pl.multiple_of(slot * rows, LANES), rows), :] = full_ref[
                    pl.ds(pl.multiple_of(block * rows_tile + q * rows, LANES), rows), :
                ]

    @pl.loop(1, n_rep)
    def _(d):
        @pl.loop(0, per_level)
        def _(i):
            @pl.when(z - d >= 0)
            def _():
                @pl.when((d < n_rep - 1) | (i < kept))
                def _():
                    arrived(d, z - d, i, up_send, above, has_up)

            @pl.when(z + d < n_rep)
            def _():
                @pl.when((d < n_rep - 1) | (i < kept))
                def _():
                    arrived(d, z + d, i, down_send, below, has_down)

    if not by_chunk:
        multiply(0, full_ref.shape[0], True)

    @pl.loop(0, chunks)
    def _(q):
        for t in range(1, n_row):
            along_row(t, q, True).wait_send()

    def drain(level, sent, sems, target):
        @pl.loop(0, sent)
        def _(i):
            block, q = block_of(level, i)
            along_rep(block, q, sems, target).wait_send()

    @pl.when(has_up)
    def _():
        @pl.loop(0, z + 1)
        def _(level):
            drain(level, jnp.where((level == 0) & (z + 1 == n_rep - 1), kept, per_level), up_send, above)

    @pl.when(has_down)
    def _():
        @pl.loop(z, n_rep)
        def _(level):
            drain(level, jnp.where((level == n_rep - 1) & (z == 1), kept, per_level), down_send, below)


def vmem():
    return pl.BlockSpec(memory_space=pltpu.VMEM)


def in_hbm(x):
    return pltpu.with_memory_space_constraint(x, pltpu.HBM)


def hbm():
    return pl.BlockSpec(memory_space=pltpu.HBM)


def handed_off(hidden, tile, shard_order, chunks, late, reorder):
    n_row, n_rep = lax.axis_size("row"), lax.axis_size("rep")
    rows_tile, cols_tile = tile.shape
    cols = cols_tile // n_row
    every = n_rep * n_row * chunks
    order = jnp.swapaxes(shard_order, 1, 2)
    dma = pltpu.SemaphoreType.DMA
    height = n_rep * n_row * rows_tile
    return pl.pallas_call(
        functools.partial(handoff_kernel, n_row, n_rep, chunks, late, reorder),
        out_shape=(
            pltpu.VMEM((height, cols), tile.dtype),
            pltpu.VMEM((hidden.shape[0], cols), jnp.float32),
            pltpu.VMEM((max(8, max(late) * (rows_tile // chunks)), cols), tile.dtype),
        ),
        in_specs=[hbm(), hbm(), hbm()],
        out_specs=(vmem(),) * 3,
        scratch_shapes=[
            pltpu.SMEM(order.shape, order.dtype),
            pltpu.VMEM((rows_tile, cols_tile), tile.dtype),
            pltpu.VMEM((n_row - 1, rows_tile, cols), tile.dtype),
            pltpu.VMEM(hidden.shape, hidden.dtype),
            dma,
            dma((chunks,)),
            dma,
            dma((n_row * chunks,)),
            dma((n_row * chunks,)),
            dma((every,)),
            dma((every,)),
            dma((every,)),
        ],
        compiler_params=pltpu.CompilerParams(
            collective_id=0, has_side_effects=True, vmem_limit_bytes=14 * MIB
        ),
    )(in_hbm(order), in_hbm(tile), in_hbm(hidden))


def store_kernel(landed_ref, served_ref, sem):
    parts = sem.shape[0]
    rows = served_ref.shape[0] // parts
    copies = [
        pltpu.make_async_copy(
            landed_ref.at[pl.ds(i * rows, rows)], served_ref.at[pl.ds(i * rows, rows)], sem.at[i]
        )
        for i in range(parts)
    ]
    for copy in copies:
        copy.start()
    for copy in copies:
        copy.wait()


def stored(landed):
    return pl.pallas_call(
        store_kernel,
        out_shape=jax.ShapeDtypeStruct(landed.shape, landed.dtype),
        in_specs=[pl.BlockSpec(memory_space=pl.ANY)],
        out_specs=pl.BlockSpec(memory_space=pl.ANY),
        scratch_shapes=[pltpu.SemaphoreType.DMA((8,))],
        compiler_params=pltpu.CompilerParams(vmem_limit_bytes=MIB),
    )(landed)


def late_kernel(
    n_row, n_rep, chunks, late,
    keep_ref, partial_ref, hidden_hbm, _, late_ref, summed_ref,
    hidden_ref, hidden_sem, send_sem, recv_sem,
):
    r, c, z = lax.axis_index("row"), lax.axis_index("col"), lax.axis_index("rep")
    slots = max(late)
    rows, cols = late_ref.shape[0] // slots, late_ref.shape[1]
    first = late_start(chunks, late)
    other = lax.rem(r + 1, n_row)
    lowest, highest = other, (n_rep - 1) * n_row + other
    gives_up, gives_down = z == n_rep - 2, z == 1
    takes_below, takes_above = z == n_rep - 1, z == 0
    above = (r, c, jnp.minimum(z + 1, n_rep - 1))
    below = (r, c, jnp.maximum(z - 1, 0))

    barrier = pltpu.get_barrier_semaphore()

    @pl.when(gives_up | takes_above)
    def _():
        pl.semaphore_signal(barrier, inc=1, device_id=above, device_id_type=MESH)

    @pl.when(gives_down | takes_below)
    def _():
        pl.semaphore_signal(barrier, inc=1, device_id=below, device_id_type=MESH)

    pl.semaphore_wait(barrier, (gives_up | takes_above).astype(jnp.int32) + (gives_down | takes_below).astype(jnp.int32))

    def moved(q, target):
        slot = q - (chunks - slots)
        return pltpu.make_async_remote_copy(
            src_ref=keep_ref.at[pl.ds(pl.multiple_of(slot * rows, LANES), rows)],
            dst_ref=late_ref.at[pl.ds(pl.multiple_of(slot * rows, LANES), rows)],
            send_sem=send_sem.at[slot],
            recv_sem=recv_sem.at[slot],
            device_id=target,
            device_id_type=MESH,
        )

    @pl.when(gives_up)
    def _():
        @pl.loop(first, chunks)
        def _(q):
            moved(q, above).start()

    @pl.when(gives_down)
    def _():
        @pl.loop(first, chunks)
        def _(q):
            moved(q, below).start()

    summed_ref[...] = partial_ref[...]
    tile = row_tiles(cols)

    def take(block, target):
        hidden_copy = pltpu.make_async_copy(
            hidden_hbm.at[:, pl.ds(pl.multiple_of((block * chunks + chunks - slots) * rows, LANES), slots * rows)],
            hidden_ref,
            hidden_sem,
        )
        hidden_copy.start()
        hidden_copy.wait()

        @pl.loop(first, chunks)
        def _(q):
            moved(q, target).wait_recv()
            within = pl.ds(pl.multiple_of((q - (chunks - slots)) * rows, LANES), rows)
            for n in range(cols // tile):
                at = pl.ds(n * tile, tile)
                summed_ref[:, at] += jnp.dot(
                    hidden_ref[:, within], late_ref[within, at], preferred_element_type=jnp.float32
                )

    @pl.when(takes_below)
    def _():
        take(lowest, below)

    @pl.when(takes_above)
    def _():
        take(highest, above)

    @pl.when(gives_up)
    def _():
        @pl.loop(first, chunks)
        def _(q):
            moved(q, above).wait_send()

    @pl.when(gives_down)
    def _():
        @pl.loop(first, chunks)
        def _(q):
            moved(q, below).wait_send()


def late_handoff(keep, partial, hidden, token, chunks, late):
    n_row, n_rep = lax.axis_size("row"), lax.axis_size("rep")
    slots = max(late)
    rows = keep.shape[0] // slots
    dma = pltpu.SemaphoreType.DMA
    return pl.pallas_call(
        functools.partial(late_kernel, n_row, n_rep, chunks, late),
        out_shape=(
            pltpu.VMEM(keep.shape, keep.dtype),
            pltpu.VMEM(partial.shape, partial.dtype),
        ),
        in_specs=[vmem(), vmem(), hbm(), hbm()],
        out_specs=(vmem(), vmem()),
        scratch_shapes=[
            pltpu.VMEM((hidden.shape[0], slots * rows), hidden.dtype),
            dma,
            dma((slots,)),
            dma((slots,)),
        ],
        cost_estimate=pl.CostEstimate(flops=10**11, bytes_accessed=10**6, transcendentals=0),
        compiler_params=pltpu.CompilerParams(
            collective_id=1, has_side_effects=True, vmem_limit_bytes=2 * MIB
        ),
    )(keep, partial, in_hbm(hidden), in_hbm(token))


def finish_kernel(n_row, n_rep, chunks, late, early_ref, late_ref, summed_ref, served_ref, projected_ref, sem, projected_sem):
    r, z = lax.axis_index("row"), lax.axis_index("rep")
    rows_tile = served_ref.shape[0] // (n_row * n_rep)
    rows = rows_tile // chunks
    slots = late_ref.shape[0] // rows
    first = late_start(chunks, late)
    block = jnp.where(z == 0, n_rep - 1, 0) * n_row + lax.rem(r + 1, n_row)
    takes = (z == 0) | (z == n_rep - 1)

    def stored(q):
        slot = q - (chunks - slots)
        return pltpu.make_async_copy(
            late_ref.at[pl.ds(pl.multiple_of(slot * rows, LANES), rows)],
            served_ref.at[pl.ds(pl.multiple_of(block * rows_tile + q * rows, LANES), rows)],
            sem.at[slot],
        )

    projected_copy = pltpu.make_async_copy(summed_ref, projected_ref, projected_sem)
    projected_copy.start()

    @pl.when(takes)
    def _():
        @pl.loop(first, chunks)
        def _(q):
            stored(q).start()

        @pl.loop(first, chunks)
        def _(q):
            stored(q).wait()

    projected_copy.wait()


def finished(early, landed, summed, chunks, late):
    n_row, n_rep = lax.axis_size("row"), lax.axis_size("rep")
    dma = pltpu.SemaphoreType.DMA
    return pl.pallas_call(
        functools.partial(finish_kernel, n_row, n_rep, chunks, late),
        out_shape=(
            jax.ShapeDtypeStruct(early.shape, early.dtype),
            jax.ShapeDtypeStruct(summed.shape, summed.dtype),
        ),
        in_specs=[pl.BlockSpec(memory_space=pl.ANY), vmem(), vmem()],
        out_specs=(pl.BlockSpec(memory_space=pl.ANY),) * 2,
        scratch_shapes=[dma((max(late),)), dma],
        input_output_aliases={0: 0},
        compiler_params=pltpu.CompilerParams(vmem_limit_bytes=MIB),
    )(early, landed, summed)


def shards(hidden, train_weight, shard_order):
    _, sub_count, n_row = shard_order.shape
    rows_tile, cols_tile = train_weight.shape
    chunks = rows_tile // LANES if rows_tile % LANES == 0 else 1
    late = LATE_CHUNKS if chunks > max(LATE_CHUNKS) and lax.axis_size("rep") > 2 else (0, 0)
    reorder = (cols_tile // (n_row * sub_count)) % LANES == 0
    tile = train_weight if reorder else ordered_pieces(train_weight, shard_order)
    landed, summed, keep = handed_off(hidden, tile, shard_order, chunks, late, reorder)
    served = stored(landed)
    if max(late) == 0:
        return served, summed
    tail, total = late_handoff(keep, summed, hidden, served, chunks, late)
    return finished(served, tail, total, chunks, late)


def solution(mesh):
    placed = (P("rep", None), P(("rep", "row"), "col"), P())
    return jax.shard_map(
        shards,
        mesh=mesh,
        in_specs=placed,
        out_specs=(P(None, ("col", "row")), P("rep", ("col", "row"))),
        check_vma=False,
    )
```

```python
import functools

import jax
import jax.numpy as jnp
from jax import lax
from jax.experimental import pallas as pl
from jax.experimental.pallas import tpu as pltpu
from jax.sharding import PartitionSpec as P

MESH = pl.DeviceIdType.MESH
LANES = 128
MIB = 1024 * 1024
LATE_CHUNKS = (1, 6)


def ordered_pieces(tile, shard_order):
    _, sub_count, row_count = shard_order.shape
    rows_tile, cols_tile = tile.shape
    piece_cols = cols_tile // row_count
    sub_cols = piece_cols // sub_count
    my_order = lax.dynamic_index_in_dim(shard_order, lax.axis_index("col"), 0, keepdims=False)
    blocks = tile.reshape(rows_tile, row_count, sub_count, sub_cols)
    pieces = []
    for s in range(row_count):
        piece = blocks[:, 0]
        for j in range(1, row_count):
            piece = jnp.where((my_order[:, s] == j)[None, :, None], blocks[:, j], piece)
        pieces.append(piece.reshape(rows_tile, piece_cols))
    return jnp.concatenate(pieces, axis=1)


def late_start(chunks, late):
    return chunks - jnp.where(lax.rem(lax.axis_index("col"), 2) == 0, late[0], late[1])


def row_tiles(cols):
    return 256 if cols % 256 == 0 else LANES


def handoff_kernel(
    n_row, n_rep, chunks, late, reorder,
    order_hbm, tile_ref, hidden_hbm, full_ref, projected_ref, keep_ref,
    order_ref, raw_ref, away_ref, hidden_ref, order_sem, raw_sem, hidden_sem, y_send, y_recv, z_recv, up_send, down_send,
):
    r, c, z = lax.axis_index("row"), lax.axis_index("col"), lax.axis_index("rep")
    rows_tile, cols_tile = tile_ref.shape
    cols = cols_tile // n_row
    rows = rows_tile // chunks
    has_up, has_down = z < n_rep - 1, z > 0
    above = (r, c, jnp.minimum(z + 1, n_rep - 1))
    below = (r, c, jnp.maximum(z - 1, 0))
    per_level = n_row * chunks
    mine = z * n_row + r
    kept = (n_row - 1) * chunks + late_start(chunks, late)

    barrier = pltpu.get_barrier_semaphore()
    for t in range(1, n_row):
        pl.semaphore_signal(barrier, inc=1, device_id=(lax.rem(r + t, n_row), c, z), device_id_type=MESH)

    @pl.when(has_up)
    def _():
        pl.semaphore_signal(barrier, inc=1, device_id=above, device_id_type=MESH)

    @pl.when(has_down)
    def _():
        pl.semaphore_signal(barrier, inc=1, device_id=below, device_id_type=MESH)

    def chunk_of(ref, block, q):
        return ref.at[pl.ds(pl.multiple_of(block * rows_tile + q * rows, 8), rows)]

    def staged(q):
        return pltpu.make_async_copy(chunk_of(tile_ref, 0, q), chunk_of(raw_ref, 0, q), raw_sem.at[q])

    order_copy = pltpu.make_async_copy(order_hbm, order_ref, order_sem)
    hidden_copy = pltpu.make_async_copy(hidden_hbm, hidden_ref, hidden_sem)
    order_copy.start()
    staged(0).start()

    sub_count = order_ref.shape[2]
    sub_cols = cols // sub_count
    step = 16 if rows % 16 == 0 else 8

    def arrange(q):
        staged(q).wait()

        @pl.loop(0, rows // step)
        def _(i):
            at = pl.ds(pl.multiple_of(q * rows + i * step, step), step)
            to = pl.ds(pl.multiple_of(mine * rows_tile + q * rows + i * step, step), step)

            def place(t, span, piece):
                if t == 0:
                    full_ref[to, span] = piece
                else:
                    away_ref[t - 1, at, span] = piece

            if reorder:
                for k in range(sub_count):
                    blocks = [raw_ref[at, pl.ds(j * cols + k * sub_cols, sub_cols)] for j in range(n_row)]
                    for t in range(n_row):
                        s = lax.rem(r + t, n_row)
                        piece = blocks[0]
                        for j in range(1, n_row):
                            piece = jnp.where(order_ref[c, s, k] == j, blocks[j], piece)
                        place(t, pl.ds(k * sub_cols, sub_cols), piece)
            else:
                for t in range(n_row):
                    s = lax.rem(r + t, n_row)
                    place(t, pl.ds(0, cols), raw_ref[at, pl.ds(pl.multiple_of(s * cols, LANES), cols)])

    def along_row(t, q, outward):
        peer = lax.rem(r + t, n_row)
        source = lax.rem(r - t + n_row, n_row)
        return pltpu.make_async_remote_copy(
            src_ref=chunk_of(away_ref.at[t - 1], 0, q),
            dst_ref=chunk_of(full_ref, z * n_row + (r if outward else source), q),
            send_sem=y_send.at[t * chunks + q],
            recv_sem=y_recv.at[t * chunks + q],
            device_id=(peer, c, z),
            device_id_type=MESH,
        )

    def along_rep(block, q, sems, target):
        return pltpu.make_async_remote_copy(
            src_ref=chunk_of(full_ref, block, q),
            dst_ref=chunk_of(full_ref, block, q),
            send_sem=sems.at[block * chunks + q],
            recv_sem=z_recv.at[block * chunks + q],
            device_id=target,
            device_id_type=MESH,
        )

    def forward(block, q):
        @pl.when(has_up)
        def _():
            along_rep(block, q, up_send, above).start()

        @pl.when(has_down)
        def _():
            along_rep(block, q, down_send, below).start()

    by_chunk = rows % LANES == 0
    tile = row_tiles(cols)

    def multiply(first, depth, fresh):
        within = pl.ds(first, depth)

        @pl.loop(0, cols // tile)
        def _(n):
            at = pl.ds(pl.multiple_of(n * tile, tile), tile)
            term = jnp.dot(hidden_ref[:, within], full_ref[within, at], preferred_element_type=jnp.float32)
            projected_ref[:, at] = term if fresh else projected_ref[:, at] + term

    def consume(block, q):
        if by_chunk:
            multiply(pl.multiple_of(block * rows_tile + q * rows, LANES), rows, False)

    def send_own(q):
        forward(mine, q)
        for t in range(1, n_row):
            along_row(t, q, True).start()

    order_copy.wait()
    arrange(0)

    @pl.loop(1, chunks)
    def _(q):
        staged(q).start()

    hidden_copy.start()
    pl.semaphore_wait(barrier, n_row - 1 + has_up.astype(jnp.int32) + has_down.astype(jnp.int32))
    send_own(0)

    @pl.loop(1, chunks)
    def _(q):
        arrange(q)

        @pl.when(q > 1)
        def _():
            send_own(q - 1)

    if chunks > 1:
        send_own(chunks - 1)

    if by_chunk:
        projected_ref[...] = jnp.zeros_like(projected_ref)
    hidden_copy.wait()

    @pl.loop(0, chunks)
    def _(q):
        consume(mine, q)

    for t in range(1, n_row):

        @pl.loop(0, chunks)
        def _(q):
            along_row(t, q, False).wait_recv()
            block = z * n_row + lax.rem(r - t + n_row, n_row)
            forward(block, q)
            consume(block, q)

    def block_of(level, i):
        return level * n_row + lax.rem(r - i // chunks + n_row, n_row), lax.rem(i, chunks)

    def arrived(d, level, i, sems, target, onward):
        block, q = block_of(level, i)
        copy = along_rep(block, q, sems, target)
        copy.wait_recv()
        deferred = (d == n_rep - 2) & (i >= kept)

        @pl.when(onward & jnp.logical_not(deferred))
        def _():
            copy.start()

        consume(block, q)
        if max(late):

            @pl.when(onward & deferred)
            def _():
                slot = q - (chunks - max(late))
                keep_ref[pl.ds(pl.multiple_of(slot * rows, LANES), rows), :] = full_ref[
                    pl.ds(pl.multiple_of(block * rows_tile + q * rows, LANES), rows), :
                ]

    @pl.loop(1, n_rep)
    def _(d):
        @pl.loop(0, per_level)
        def _(i):
            @pl.when(z - d >= 0)
            def _():
                @pl.when((d < n_rep - 1) | (i < kept))
                def _():
                    arrived(d, z - d, i, up_send, above, has_up)

            @pl.when(z + d < n_rep)
            def _():
                @pl.when((d < n_rep - 1) | (i < kept))
                def _():
                    arrived(d, z + d, i, down_send, below, has_down)

    if not by_chunk:
        multiply(0, full_ref.shape[0], True)

    @pl.loop(0, chunks)
    def _(q):
        for t in range(1, n_row):
            along_row(t, q, True).wait_send()

    def drain(level, sent, sems, target):
        @pl.loop(0, sent)
        def _(i):
            block, q = block_of(level, i)
            along_rep(block, q, sems, target).wait_send()

    @pl.when(has_up)
    def _():
        @pl.loop(0, z + 1)
        def _(level):
            drain(level, jnp.where((level == 0) & (z + 1 == n_rep - 1), kept, per_level), up_send, above)

    @pl.when(has_down)
    def _():
        @pl.loop(z, n_rep)
        def _(level):
            drain(level, jnp.where((level == n_rep - 1) & (z == 1), kept, per_level), down_send, below)


def vmem():
    return pl.BlockSpec(memory_space=pltpu.VMEM)


def in_hbm(x):
    return pltpu.with_memory_space_constraint(x, pltpu.HBM)


def hbm():
    return pl.BlockSpec(memory_space=pltpu.HBM)


def handed_off(hidden, tile, shard_order, chunks, late, reorder):
    n_row, n_rep = lax.axis_size("row"), lax.axis_size("rep")
    rows_tile, cols_tile = tile.shape
    cols = cols_tile // n_row
    every = n_rep * n_row * chunks
    order = jnp.swapaxes(shard_order, 1, 2)
    dma = pltpu.SemaphoreType.DMA
    height = n_rep * n_row * rows_tile
    return pl.pallas_call(
        functools.partial(handoff_kernel, n_row, n_rep, chunks, late, reorder),
        out_shape=(
            pltpu.VMEM((height, cols), tile.dtype),
            pltpu.VMEM((hidden.shape[0], cols), jnp.float32),
            pltpu.VMEM((max(8, max(late) * (rows_tile // chunks)), cols), tile.dtype),
        ),
        in_specs=[hbm(), hbm(), hbm()],
        out_specs=(vmem(),) * 3,
        scratch_shapes=[
            pltpu.SMEM(order.shape, order.dtype),
            pltpu.VMEM((rows_tile, cols_tile), tile.dtype),
            pltpu.VMEM((n_row - 1, rows_tile, cols), tile.dtype),
            pltpu.VMEM(hidden.shape, hidden.dtype),
            dma,
            dma((chunks,)),
            dma,
            dma((n_row * chunks,)),
            dma((n_row * chunks,)),
            dma((every,)),
            dma((every,)),
            dma((every,)),
        ],
        compiler_params=pltpu.CompilerParams(
            collective_id=0, has_side_effects=True, vmem_limit_bytes=14 * MIB
        ),
    )(in_hbm(order), in_hbm(tile), in_hbm(hidden))


def store_kernel(landed_ref, served_ref, sem):
    parts = sem.shape[0]
    rows = served_ref.shape[0] // parts
    copies = [
        pltpu.make_async_copy(
            landed_ref.at[pl.ds(i * rows, rows)], served_ref.at[pl.ds(i * rows, rows)], sem.at[i]
        )
        for i in range(parts)
    ]
    for copy in copies:
        copy.start()
    for copy in copies:
        copy.wait()


def stored(landed):
    return pl.pallas_call(
        store_kernel,
        out_shape=jax.ShapeDtypeStruct(landed.shape, landed.dtype),
        in_specs=[pl.BlockSpec(memory_space=pl.ANY)],
        out_specs=pl.BlockSpec(memory_space=pl.ANY),
        scratch_shapes=[pltpu.SemaphoreType.DMA((8,))],
        compiler_params=pltpu.CompilerParams(vmem_limit_bytes=MIB),
    )(landed)


def late_kernel(
    n_row, n_rep, chunks, late,
    keep_ref, partial_ref, hidden_hbm, _, late_ref, summed_ref,
    hidden_ref, hidden_sem, send_sem, recv_sem,
):
    r, c, z = lax.axis_index("row"), lax.axis_index("col"), lax.axis_index("rep")
    slots = max(late)
    rows, cols = late_ref.shape[0] // slots, late_ref.shape[1]
    first = late_start(chunks, late)
    other = lax.rem(r + 1, n_row)
    lowest, highest = other, (n_rep - 1) * n_row + other
    gives_up, gives_down = z == n_rep - 2, z == 1
    takes_below, takes_above = z == n_rep - 1, z == 0
    above = (r, c, jnp.minimum(z + 1, n_rep - 1))
    below = (r, c, jnp.maximum(z - 1, 0))

    barrier = pltpu.get_barrier_semaphore()

    @pl.when(gives_up | takes_above)
    def _():
        pl.semaphore_signal(barrier, inc=1, device_id=above, device_id_type=MESH)

    @pl.when(gives_down | takes_below)
    def _():
        pl.semaphore_signal(barrier, inc=1, device_id=below, device_id_type=MESH)

    pl.semaphore_wait(barrier, (gives_up | takes_above).astype(jnp.int32) + (gives_down | takes_below).astype(jnp.int32))

    def moved(q, target):
        slot = q - (chunks - slots)
        return pltpu.make_async_remote_copy(
            src_ref=keep_ref.at[pl.ds(pl.multiple_of(slot * rows, LANES), rows)],
            dst_ref=late_ref.at[pl.ds(pl.multiple_of(slot * rows, LANES), rows)],
            send_sem=send_sem.at[slot],
            recv_sem=recv_sem.at[slot],
            device_id=target,
            device_id_type=MESH,
        )

    @pl.when(gives_up)
    def _():
        @pl.loop(first, chunks)
        def _(q):
            moved(q, above).start()

    @pl.when(gives_down)
    def _():
        @pl.loop(first, chunks)
        def _(q):
            moved(q, below).start()

    summed_ref[...] = partial_ref[...]
    tile = row_tiles(cols)

    def take(block, target):
        hidden_copy = pltpu.make_async_copy(
            hidden_hbm.at[:, pl.ds(pl.multiple_of((block * chunks + chunks - slots) * rows, LANES), slots * rows)],
            hidden_ref,
            hidden_sem,
        )
        hidden_copy.start()
        hidden_copy.wait()

        @pl.loop(first, chunks)
        def _(q):
            moved(q, target).wait_recv()
            within = pl.ds(pl.multiple_of((q - (chunks - slots)) * rows, LANES), rows)
            for n in range(cols // tile):
                at = pl.ds(n * tile, tile)
                summed_ref[:, at] += jnp.dot(
                    hidden_ref[:, within], late_ref[within, at], preferred_element_type=jnp.float32
                )

    @pl.when(takes_below)
    def _():
        take(lowest, below)

    @pl.when(takes_above)
    def _():
        take(highest, above)

    @pl.when(gives_up)
    def _():
        @pl.loop(first, chunks)
        def _(q):
            moved(q, above).wait_send()

    @pl.when(gives_down)
    def _():
        @pl.loop(first, chunks)
        def _(q):
            moved(q, below).wait_send()


def late_handoff(keep, partial, hidden, token, chunks, late):
    n_row, n_rep = lax.axis_size("row"), lax.axis_size("rep")
    slots = max(late)
    rows = keep.shape[0] // slots
    dma = pltpu.SemaphoreType.DMA
    return pl.pallas_call(
        functools.partial(late_kernel, n_row, n_rep, chunks, late),
        out_shape=(
            pltpu.VMEM(keep.shape, keep.dtype),
            pltpu.VMEM(partial.shape, partial.dtype),
        ),
        in_specs=[vmem(), vmem(), hbm(), hbm()],
        out_specs=(vmem(), vmem()),
        scratch_shapes=[
            pltpu.VMEM((hidden.shape[0], slots * rows), hidden.dtype),
            dma,
            dma((slots,)),
            dma((slots,)),
        ],
        cost_estimate=pl.CostEstimate(flops=10**11, bytes_accessed=10**6, transcendentals=0),
        compiler_params=pltpu.CompilerParams(
            collective_id=1, has_side_effects=True, vmem_limit_bytes=2 * MIB
        ),
    )(keep, partial, in_hbm(hidden), in_hbm(token))


def finish_kernel(n_row, n_rep, chunks, late, early_ref, late_ref, summed_ref, served_ref, projected_ref, sem, projected_sem):
    r, z = lax.axis_index("row"), lax.axis_index("rep")
    rows_tile = served_ref.shape[0] // (n_row * n_rep)
    rows = rows_tile // chunks
    slots = late_ref.shape[0] // rows
    first = late_start(chunks, late)
    block = jnp.where(z == 0, n_rep - 1, 0) * n_row + lax.rem(r + 1, n_row)
    takes = (z == 0) | (z == n_rep - 1)

    def stored(q):
        slot = q - (chunks - slots)
        return pltpu.make_async_copy(
            late_ref.at[pl.ds(pl.multiple_of(slot * rows, LANES), rows)],
            served_ref.at[pl.ds(pl.multiple_of(block * rows_tile + q * rows, LANES), rows)],
            sem.at[slot],
        )

    projected_copy = pltpu.make_async_copy(summed_ref, projected_ref, projected_sem)
    projected_copy.start()

    @pl.when(takes)
    def _():
        @pl.loop(first, chunks)
        def _(q):
            stored(q).start()

        @pl.loop(first, chunks)
        def _(q):
            stored(q).wait()

    projected_copy.wait()


def finished(early, landed, summed, chunks, late):
    n_row, n_rep = lax.axis_size("row"), lax.axis_size("rep")
    dma = pltpu.SemaphoreType.DMA
    return pl.pallas_call(
        functools.partial(finish_kernel, n_row, n_rep, chunks, late),
        out_shape=(
            jax.ShapeDtypeStruct(early.shape, early.dtype),
            jax.ShapeDtypeStruct(summed.shape, summed.dtype),
        ),
        in_specs=[pl.BlockSpec(memory_space=pl.ANY), vmem(), vmem()],
        out_specs=(pl.BlockSpec(memory_space=pl.ANY),) * 2,
        scratch_shapes=[dma((max(late),)), dma],
        input_output_aliases={0: 0},
        compiler_params=pltpu.CompilerParams(vmem_limit_bytes=MIB),
    )(early, landed, summed)


def shards(hidden, train_weight, shard_order):
    _, sub_count, n_row = shard_order.shape
    rows_tile, cols_tile = train_weight.shape
    chunks = rows_tile // LANES if rows_tile % LANES == 0 else 1
    late = LATE_CHUNKS if chunks > max(LATE_CHUNKS) and lax.axis_size("rep") > 3 else (0, 0)
    reorder = (cols_tile // (n_row * sub_count)) % LANES == 0
    tile = train_weight if reorder else ordered_pieces(train_weight, shard_order)
    landed, summed, keep = handed_off(hidden, tile, shard_order, chunks, late, reorder)
    served = stored(landed)
    if max(late) == 0:
        return served, summed
    tail, total = late_handoff(keep, summed, hidden, served, chunks, late)
    return finished(served, tail, total, chunks, late)


def solution(mesh):
    placed = (P("rep", None), P(("rep", "row"), "col"), P())
    return jax.shard_map(
        shards,
        mesh=mesh,
        in_specs=placed,
        out_specs=(P(None, ("col", "row")), P("rep", ("col", "row"))),
        check_vma=False,
    )
```

```python
import functools

import jax
import jax.numpy as jnp
from jax import lax
from jax.experimental import pallas as pl
from jax.experimental.pallas import tpu as pltpu
from jax.sharding import PartitionSpec as P

MESH = pl.DeviceIdType.MESH
LANES = 128
MIB = 1024 * 1024
LATE_CHUNKS = (1, 6)
FIRST_CHUNKS = (3, 1)


def ordered_pieces(tile, shard_order):
    _, sub_count, row_count = shard_order.shape
    rows_tile, cols_tile = tile.shape
    piece_cols = cols_tile // row_count
    sub_cols = piece_cols // sub_count
    my_order = lax.dynamic_index_in_dim(shard_order, lax.axis_index("col"), 0, keepdims=False)
    blocks = tile.reshape(rows_tile, row_count, sub_count, sub_cols)
    pieces = []
    for s in range(row_count):
        piece = blocks[:, 0]
        for j in range(1, row_count):
            piece = jnp.where((my_order[:, s] == j)[None, :, None], blocks[:, j], piece)
        pieces.append(piece.reshape(rows_tile, piece_cols))
    return jnp.concatenate(pieces, axis=1)


def by_core(pair):
    return jnp.where(lax.rem(lax.axis_index("col"), 2) == 0, pair[0], pair[1])


def late_start(chunks, late):
    return chunks - by_core(late)


def row_tiles(cols):
    return 256 if cols % 256 == 0 else LANES


def step_of(rows):
    return 16 if rows % 16 == 0 else 8


def arrange_rows(order_ref, raw_ref, n_row, first, rows, reorder, shifts, place):
    r, c = lax.axis_index("row"), lax.axis_index("col")
    cols = raw_ref.shape[1] // n_row
    sub_count = order_ref.shape[2]
    sub_cols = cols // sub_count
    step = step_of(rows)

    @pl.loop(0, rows // step)
    def _(i):
        to = first + i * step
        at = pl.ds(pl.multiple_of(to, step), step)
        if reorder:
            for k in range(sub_count):
                blocks = [raw_ref[at, pl.ds(j * cols + k * sub_cols, sub_cols)] for j in range(n_row)]
                for t in shifts:
                    s = lax.rem(r + t, n_row)
                    piece = blocks[0]
                    for j in range(1, n_row):
                        piece = jnp.where(order_ref[c, s, k] == j, blocks[j], piece)
                    place(t, to, pl.ds(k * sub_cols, sub_cols), piece)
        else:
            for t in shifts:
                s = lax.rem(r + t, n_row)
                place(t, to, pl.ds(0, cols), raw_ref[at, pl.ds(pl.multiple_of(s * cols, LANES), cols)])


def edges(n_rep):
    z = lax.axis_index("rep")
    return z == n_rep - 2, z == 1, z == n_rep - 1, z == 0


def pair_barrier(n_rep, above, below):
    gives_up, gives_down, takes_below, takes_above = edges(n_rep)
    barrier = pltpu.get_barrier_semaphore()

    @pl.when(gives_up | takes_above)
    def _():
        pl.semaphore_signal(barrier, inc=1, device_id=above, device_id_type=MESH)

    @pl.when(gives_down | takes_below)
    def _():
        pl.semaphore_signal(barrier, inc=1, device_id=below, device_id_type=MESH)

    return barrier, (gives_up | takes_above).astype(jnp.int32) + (gives_down | takes_below).astype(jnp.int32)


def first_kernel(
    n_row, n_rep, chunks, first, reorder,
    order_hbm, tile_ref, landed_ref, order_ref, raw_ref, own_ref, order_sem, raw_sem, send_sem, recv_sem,
):
    r, c, z = lax.axis_index("row"), lax.axis_index("col"), lax.axis_index("rep")
    rows = tile_ref.shape[0] // chunks
    count = by_core(first)
    gives_up, gives_down, takes_below, takes_above = edges(n_rep)
    above = (r, c, jnp.minimum(z + 1, n_rep - 1))
    below = (r, c, jnp.maximum(z - 1, 0))
    barrier, expected = pair_barrier(n_rep, above, below)

    parts = 4 if rows % 64 == 0 else 1
    part = rows // parts

    def chunk_of(ref, q, i=None):
        if i is None:
            return ref.at[pl.ds(pl.multiple_of(q * rows, 8), rows)]
        return ref.at[pl.ds(pl.multiple_of(q * rows + i * part, 8), part)]

    def staged(q):
        return pltpu.make_async_copy(chunk_of(tile_ref, q), chunk_of(raw_ref, q), raw_sem.at[parts + q])

    def staged_part(i):
        return pltpu.make_async_copy(chunk_of(tile_ref, 0, i), chunk_of(raw_ref, 0, i), raw_sem.at[i])

    def moved(q, target, i=None):
        return pltpu.make_async_remote_copy(
            src_ref=chunk_of(own_ref, q, i),
            dst_ref=chunk_of(landed_ref, q, i),
            send_sem=send_sem.at[q],
            recv_sem=recv_sem.at[q],
            device_id=target,
            device_id_type=MESH,
        )

    def place(t, to, span, piece):
        own_ref[pl.ds(pl.multiple_of(to, 8), step_of(rows)), span] = piece

    gives = gives_up | gives_down

    def arrange(first, height):
        arrange_rows(order_ref, raw_ref, n_row, first, height, reorder, (0,), place)

    @pl.when(gives)
    def _():
        order_copy = pltpu.make_async_copy(order_hbm, order_ref, order_sem)
        order_copy.start()

        @pl.loop(0, parts)
        def _(i):
            staged_part(i).start()

        order_copy.wait()
        staged_part(0).wait()
        arrange(0, part)

        @pl.loop(1, count)
        def _(q):
            staged(q).start()

    @pl.when(expected > 0)
    def _():
        pl.semaphore_wait(barrier, expected)

    def send(q, i=None):
        @pl.when(gives_up)
        def _():
            moved(q, above, i).start()

        @pl.when(gives_down)
        def _():
            moved(q, below, i).start()

    @pl.when(gives)
    def _():
        send(0, 0)

        @pl.loop(1, parts)
        def _(i):
            staged_part(i).wait()
            arrange(i * part, part)

        @pl.loop(1, parts)
        def _(i):
            send(0, i)

        @pl.loop(1, count)
        def _(q):
            staged(q).wait()
            arrange(q * rows, rows)

        @pl.loop(1, count)
        def _(q):
            send(q)

        @pl.loop(0, count)
        def _(q):
            @pl.when(gives_up)
            def _():
                moved(q, above).wait_send()

            @pl.when(gives_down)
            def _():
                moved(q, below).wait_send()

    @pl.when(takes_below)
    def _():
        @pl.loop(0, count)
        def _(q):
            moved(q, below).wait_recv()

    @pl.when(takes_above)
    def _():
        @pl.loop(0, count)
        def _(q):
            moved(q, above).wait_recv()


def first_handoff(tile, order, cols, chunks, first, reorder):
    n_row, n_rep = lax.axis_size("row"), lax.axis_size("rep")
    slots = max(first)
    height = slots * (tile.shape[0] // chunks)
    dma = pltpu.SemaphoreType.DMA
    return pl.pallas_call(
        functools.partial(first_kernel, n_row, n_rep, chunks, first, reorder),
        out_shape=pltpu.VMEM((height, cols), tile.dtype),
        in_specs=[hbm(), hbm()],
        out_specs=vmem(),
        scratch_shapes=[
            pltpu.SMEM(order.shape, order.dtype),
            pltpu.VMEM((height, tile.shape[1]), tile.dtype),
            pltpu.VMEM((height, cols), tile.dtype),
            dma,
            dma((slots + 4,)),
            dma((slots,)),
            dma((slots,)),
        ],
        compiler_params=pltpu.CompilerParams(
            collective_id=2, has_side_effects=True, vmem_limit_bytes=6 * MIB
        ),
    )(in_hbm(order), in_hbm(tile))


def handoff_kernel(
    n_row, n_rep, chunks, late, first, reorder,
    order_hbm, tile_ref, hidden_hbm, landed_ref, full_ref, projected_ref, keep_ref,
    order_ref, raw_ref, away_ref, hidden_ref, order_sem, raw_sem, hidden_sem, y_send, y_recv, z_recv, up_send, down_send,
):
    r, c, z = lax.axis_index("row"), lax.axis_index("col"), lax.axis_index("rep")
    rows_tile, cols_tile = tile_ref.shape
    cols = cols_tile // n_row
    rows = rows_tile // chunks
    has_up, has_down = z < n_rep - 1, z > 0
    above = (r, c, jnp.minimum(z + 1, n_rep - 1))
    below = (r, c, jnp.maximum(z - 1, 0))
    per_level = n_row * chunks
    mine = z * n_row + r
    kept = (n_row - 1) * chunks + late_start(chunks, late)
    gives_up, gives_down, takes_below, takes_above = edges(n_rep)
    ahead = by_core(first)
    up_from, down_from = jnp.where(gives_up, ahead, 0), jnp.where(gives_down, ahead, 0)

    barrier = pltpu.get_barrier_semaphore()
    for t in range(1, n_row):
        pl.semaphore_signal(barrier, inc=1, device_id=(lax.rem(r + t, n_row), c, z), device_id_type=MESH)

    @pl.when(has_up)
    def _():
        pl.semaphore_signal(barrier, inc=1, device_id=above, device_id_type=MESH)

    @pl.when(has_down)
    def _():
        pl.semaphore_signal(barrier, inc=1, device_id=below, device_id_type=MESH)

    def chunk_of(ref, block, q):
        return ref.at[pl.ds(pl.multiple_of(block * rows_tile + q * rows, 8), rows)]

    def staged(q):
        return pltpu.make_async_copy(chunk_of(tile_ref, 0, q), chunk_of(raw_ref, 0, q), raw_sem.at[q])

    order_copy = pltpu.make_async_copy(order_hbm, order_ref, order_sem)
    hidden_copy = pltpu.make_async_copy(hidden_hbm, hidden_ref, hidden_sem)
    order_copy.start()
    staged(0).start()

    def place(t, to, span, piece):
        if t == 0:
            full_ref[pl.ds(pl.multiple_of(mine * rows_tile + to, 8), step), span] = piece
        else:
            away_ref[t - 1, pl.ds(pl.multiple_of(to, 8), step), span] = piece

    step = step_of(rows)

    def arrange(q):
        staged(q).wait()
        arrange_rows(order_ref, raw_ref, n_row, q * rows, rows, reorder, range(n_row), place)

    def along_row(t, q, outward):
        peer = lax.rem(r + t, n_row)
        source = lax.rem(r - t + n_row, n_row)
        return pltpu.make_async_remote_copy(
            src_ref=chunk_of(away_ref.at[t - 1], 0, q),
            dst_ref=chunk_of(full_ref, z * n_row + (r if outward else source), q),
            send_sem=y_send.at[t * chunks + q],
            recv_sem=y_recv.at[t * chunks + q],
            device_id=(peer, c, z),
            device_id_type=MESH,
        )

    def along_rep(block, q, sems, target):
        return pltpu.make_async_remote_copy(
            src_ref=chunk_of(full_ref, block, q),
            dst_ref=chunk_of(full_ref, block, q),
            send_sem=sems.at[block * chunks + q],
            recv_sem=z_recv.at[block * chunks + q],
            device_id=target,
            device_id_type=MESH,
        )

    def forward(block, q, up=True, down=True):
        @pl.when(has_up & up)
        def _():
            along_rep(block, q, up_send, above).start()

        @pl.when(has_down & down)
        def _():
            along_rep(block, q, down_send, below).start()

    by_chunk = rows % LANES == 0
    tile = row_tiles(cols)

    def multiply(first, depth, fresh):
        within = pl.ds(first, depth)

        @pl.loop(0, cols // tile)
        def _(n):
            at = pl.ds(pl.multiple_of(n * tile, tile), tile)
            term = jnp.dot(hidden_ref[:, within], full_ref[within, at], preferred_element_type=jnp.float32)
            projected_ref[:, at] = term if fresh else projected_ref[:, at] + term

    def consume(block, q):
        if by_chunk:
            multiply(pl.multiple_of(block * rows_tile + q * rows, LANES), rows, False)

    def send_own(q):
        forward(mine, q, q >= up_from, q >= down_from)
        for t in range(1, n_row):
            along_row(t, q, True).start()

    order_copy.wait()
    arrange(0)

    @pl.loop(1, chunks)
    def _(q):
        staged(q).start()

    hidden_copy.start()
    pl.semaphore_wait(barrier, n_row - 1 + has_up.astype(jnp.int32) + has_down.astype(jnp.int32))
    send_own(0)

    @pl.loop(1, chunks)
    def _(q):
        arrange(q)

        @pl.when(q > 1)
        def _():
            send_own(q - 1)

    if chunks > 1:
        send_own(chunks - 1)

    if by_chunk:
        projected_ref[...] = jnp.zeros_like(projected_ref)
    hidden_copy.wait()

    @pl.loop(0, chunks)
    def _(q):
        consume(mine, q)

    for t in range(1, n_row):

        @pl.loop(0, chunks)
        def _(q):
            along_row(t, q, False).wait_recv()
            block = z * n_row + lax.rem(r - t + n_row, n_row)
            forward(block, q)
            consume(block, q)

    def block_of(level, i):
        return level * n_row + lax.rem(r - i // chunks + n_row, n_row), lax.rem(i, chunks)

    def arrived(d, level, i, sems, target, onward):
        block, q = block_of(level, i)
        copy = along_rep(block, q, sems, target)
        taken = (d == 1) & (i < ahead) & jnp.logical_not(onward)

        @pl.when(jnp.logical_not(taken))
        def _():
            copy.wait_recv()

        if max(first):

            @pl.when(taken)
            def _():
                full_ref[pl.ds(pl.multiple_of(block * rows_tile + q * rows, LANES), rows), :] = landed_ref[
                    pl.ds(pl.multiple_of(jnp.minimum(q, max(first) - 1) * rows, LANES), rows), :
                ]

        deferred = (d == n_rep - 2) & (i >= kept)

        @pl.when(onward & jnp.logical_not(deferred))
        def _():
            copy.start()

        consume(block, q)
        if max(late):

            @pl.when(onward & deferred)
            def _():
                slot = q - (chunks - max(late))
                keep_ref[pl.ds(pl.multiple_of(slot * rows, LANES), rows), :] = full_ref[
                    pl.ds(pl.multiple_of(block * rows_tile + q * rows, LANES), rows), :
                ]

    @pl.loop(1, n_rep)
    def _(d):
        @pl.loop(0, per_level)
        def _(i):
            @pl.when(z - d >= 0)
            def _():
                @pl.when((d < n_rep - 1) | (i < kept))
                def _():
                    arrived(d, z - d, i, up_send, above, has_up)

            @pl.when(z + d < n_rep)
            def _():
                @pl.when((d < n_rep - 1) | (i < kept))
                def _():
                    arrived(d, z + d, i, down_send, below, has_down)

    if not by_chunk:
        multiply(0, full_ref.shape[0], True)

    @pl.loop(0, chunks)
    def _(q):
        for t in range(1, n_row):
            along_row(t, q, True).wait_send()

    def drain(level, begin, sent, sems, target):
        @pl.loop(begin, sent)
        def _(i):
            block, q = block_of(level, i)
            along_rep(block, q, sems, target).wait_send()

    @pl.when(has_up)
    def _():
        @pl.loop(0, z + 1)
        def _(level):
            drain(level, jnp.where(level == z, up_from, 0), jnp.where((level == 0) & gives_up, kept, per_level), up_send, above)

    @pl.when(has_down)
    def _():
        @pl.loop(z, n_rep)
        def _(level):
            drain(level, jnp.where(level == z, down_from, 0), jnp.where((level == n_rep - 1) & gives_down, kept, per_level), down_send, below)


def vmem():
    return pl.BlockSpec(memory_space=pltpu.VMEM)


def in_hbm(x):
    return pltpu.with_memory_space_constraint(x, pltpu.HBM)


def hbm():
    return pl.BlockSpec(memory_space=pltpu.HBM)


def handed_off(hidden, tile, order, chunks, late, first, reorder):
    n_row, n_rep = lax.axis_size("row"), lax.axis_size("rep")
    rows_tile, cols_tile = tile.shape
    cols = cols_tile // n_row
    every = n_rep * n_row * chunks
    if max(first):
        landed = first_handoff(tile, order, cols, chunks, first, reorder)
    else:
        landed = jnp.zeros((8, cols), tile.dtype)
    dma = pltpu.SemaphoreType.DMA
    height = n_rep * n_row * rows_tile
    return pl.pallas_call(
        functools.partial(handoff_kernel, n_row, n_rep, chunks, late, first, reorder),
        out_shape=(
            pltpu.VMEM((height, cols), tile.dtype),
            pltpu.VMEM((hidden.shape[0], cols), jnp.float32),
            pltpu.VMEM((max(8, max(late) * (rows_tile // chunks)), cols), tile.dtype),
        ),
        in_specs=[hbm(), hbm(), hbm(), vmem()],
        out_specs=(vmem(),) * 3,
        scratch_shapes=[
            pltpu.SMEM(order.shape, order.dtype),
            pltpu.VMEM((rows_tile, cols_tile), tile.dtype),
            pltpu.VMEM((n_row - 1, rows_tile, cols), tile.dtype),
            pltpu.VMEM(hidden.shape, hidden.dtype),
            dma,
            dma((chunks,)),
            dma,
            dma((n_row * chunks,)),
            dma((n_row * chunks,)),
            dma((every,)),
            dma((every,)),
            dma((every,)),
        ],
        compiler_params=pltpu.CompilerParams(
            collective_id=0, has_side_effects=True, vmem_limit_bytes=14 * MIB
        ),
    )(in_hbm(order), in_hbm(tile), in_hbm(hidden), landed)


def store_kernel(landed_ref, served_ref, sem):
    parts = sem.shape[0]
    rows = served_ref.shape[0] // parts
    copies = [
        pltpu.make_async_copy(
            landed_ref.at[pl.ds(i * rows, rows)], served_ref.at[pl.ds(i * rows, rows)], sem.at[i]
        )
        for i in range(parts)
    ]
    for copy in copies:
        copy.start()
    for copy in copies:
        copy.wait()


def stored(landed):
    return pl.pallas_call(
        store_kernel,
        out_shape=jax.ShapeDtypeStruct(landed.shape, landed.dtype),
        in_specs=[pl.BlockSpec(memory_space=pl.ANY)],
        out_specs=pl.BlockSpec(memory_space=pl.ANY),
        scratch_shapes=[pltpu.SemaphoreType.DMA((8,))],
        compiler_params=pltpu.CompilerParams(vmem_limit_bytes=MIB),
    )(landed)


def late_kernel(
    n_row, n_rep, chunks, late,
    keep_ref, partial_ref, hidden_hbm, _, late_ref, summed_ref,
    hidden_ref, hidden_sem, send_sem, recv_sem,
):
    r, c, z = lax.axis_index("row"), lax.axis_index("col"), lax.axis_index("rep")
    slots = max(late)
    rows, cols = late_ref.shape[0] // slots, late_ref.shape[1]
    first = late_start(chunks, late)
    other = lax.rem(r + 1, n_row)
    lowest, highest = other, (n_rep - 1) * n_row + other
    gives_up, gives_down, takes_below, takes_above = edges(n_rep)
    above = (r, c, jnp.minimum(z + 1, n_rep - 1))
    below = (r, c, jnp.maximum(z - 1, 0))

    barrier, expected = pair_barrier(n_rep, above, below)
    pl.semaphore_wait(barrier, expected)

    def moved(q, target):
        slot = q - (chunks - slots)
        return pltpu.make_async_remote_copy(
            src_ref=keep_ref.at[pl.ds(pl.multiple_of(slot * rows, LANES), rows)],
            dst_ref=late_ref.at[pl.ds(pl.multiple_of(slot * rows, LANES), rows)],
            send_sem=send_sem.at[slot],
            recv_sem=recv_sem.at[slot],
            device_id=target,
            device_id_type=MESH,
        )

    @pl.when(gives_up)
    def _():
        @pl.loop(first, chunks)
        def _(q):
            moved(q, above).start()

    @pl.when(gives_down)
    def _():
        @pl.loop(first, chunks)
        def _(q):
            moved(q, below).start()

    summed_ref[...] = partial_ref[...]
    tile = row_tiles(cols)

    def take(block, target):
        hidden_copy = pltpu.make_async_copy(
            hidden_hbm.at[:, pl.ds(pl.multiple_of((block * chunks + chunks - slots) * rows, LANES), slots * rows)],
            hidden_ref,
            hidden_sem,
        )
        hidden_copy.start()
        hidden_copy.wait()

        @pl.loop(first, chunks)
        def _(q):
            moved(q, target).wait_recv()
            within = pl.ds(pl.multiple_of((q - (chunks - slots)) * rows, LANES), rows)
            for n in range(cols // tile):
                at = pl.ds(n * tile, tile)
                summed_ref[:, at] += jnp.dot(
                    hidden_ref[:, within], late_ref[within, at], preferred_element_type=jnp.float32
                )

    @pl.when(takes_below)
    def _():
        take(lowest, below)

    @pl.when(takes_above)
    def _():
        take(highest, above)

    @pl.when(gives_up)
    def _():
        @pl.loop(first, chunks)
        def _(q):
            moved(q, above).wait_send()

    @pl.when(gives_down)
    def _():
        @pl.loop(first, chunks)
        def _(q):
            moved(q, below).wait_send()


def late_handoff(keep, partial, hidden, token, chunks, late):
    n_row, n_rep = lax.axis_size("row"), lax.axis_size("rep")
    slots = max(late)
    rows = keep.shape[0] // slots
    dma = pltpu.SemaphoreType.DMA
    return pl.pallas_call(
        functools.partial(late_kernel, n_row, n_rep, chunks, late),
        out_shape=(
            pltpu.VMEM(keep.shape, keep.dtype),
            pltpu.VMEM(partial.shape, partial.dtype),
        ),
        in_specs=[vmem(), vmem(), hbm(), hbm()],
        out_specs=(vmem(), vmem()),
        scratch_shapes=[
            pltpu.VMEM((hidden.shape[0], slots * rows), hidden.dtype),
            dma,
            dma((slots,)),
            dma((slots,)),
        ],
        cost_estimate=pl.CostEstimate(flops=10**11, bytes_accessed=10**6, transcendentals=0),
        compiler_params=pltpu.CompilerParams(
            collective_id=1, has_side_effects=True, vmem_limit_bytes=2 * MIB
        ),
    )(keep, partial, in_hbm(hidden), in_hbm(token))


def finish_kernel(n_row, n_rep, chunks, late, early_ref, late_ref, summed_ref, served_ref, projected_ref, sem, projected_sem):
    r, z = lax.axis_index("row"), lax.axis_index("rep")
    rows_tile = served_ref.shape[0] // (n_row * n_rep)
    rows = rows_tile // chunks
    slots = late_ref.shape[0] // rows
    first = late_start(chunks, late)
    block = jnp.where(z == 0, n_rep - 1, 0) * n_row + lax.rem(r + 1, n_row)
    takes = (z == 0) | (z == n_rep - 1)

    def stored(q):
        slot = q - (chunks - slots)
        return pltpu.make_async_copy(
            late_ref.at[pl.ds(pl.multiple_of(slot * rows, LANES), rows)],
            served_ref.at[pl.ds(pl.multiple_of(block * rows_tile + q * rows, LANES), rows)],
            sem.at[slot],
        )

    projected_copy = pltpu.make_async_copy(summed_ref, projected_ref, projected_sem)
    projected_copy.start()

    @pl.when(takes)
    def _():
        @pl.loop(first, chunks)
        def _(q):
            stored(q).start()

        @pl.loop(first, chunks)
        def _(q):
            stored(q).wait()

    projected_copy.wait()


def finished(early, landed, summed, chunks, late):
    n_row, n_rep = lax.axis_size("row"), lax.axis_size("rep")
    dma = pltpu.SemaphoreType.DMA
    return pl.pallas_call(
        functools.partial(finish_kernel, n_row, n_rep, chunks, late),
        out_shape=(
            jax.ShapeDtypeStruct(early.shape, early.dtype),
            jax.ShapeDtypeStruct(summed.shape, summed.dtype),
        ),
        in_specs=[pl.BlockSpec(memory_space=pl.ANY), vmem(), vmem()],
        out_specs=(pl.BlockSpec(memory_space=pl.ANY),) * 2,
        scratch_shapes=[dma((max(late),)), dma],
        input_output_aliases={0: 0},
        compiler_params=pltpu.CompilerParams(vmem_limit_bytes=MIB),
    )(early, landed, summed)


def shards(hidden, train_weight, shard_order):
    _, sub_count, n_row = shard_order.shape
    rows_tile, cols_tile = train_weight.shape
    chunks = rows_tile // LANES if rows_tile % LANES == 0 else 1
    split = chunks > max(LATE_CHUNKS + FIRST_CHUNKS) and lax.axis_size("rep") > 3
    late = LATE_CHUNKS if split else (0, 0)
    first = FIRST_CHUNKS if split else (0, 0)
    reorder = (cols_tile // (n_row * sub_count)) % LANES == 0
    tile = train_weight if reorder else ordered_pieces(train_weight, shard_order)
    landed, summed, keep = handed_off(hidden, tile, jnp.swapaxes(shard_order, 1, 2), chunks, late, first, reorder)
    served = stored(landed)
    if max(late) == 0:
        return served, summed
    tail, total = late_handoff(keep, summed, hidden, served, chunks, late)
    return finished(served, tail, total, chunks, late)


def solution(mesh):
    placed = (P("rep", None), P(("rep", "row"), "col"), P())
    return jax.shard_map(
        shards,
        mesh=mesh,
        in_specs=placed,
        out_specs=(P(None, ("col", "row")), P("rep", ("col", "row"))),
        check_vma=False,
    )
```

```python
import functools

import jax
import jax.numpy as jnp
from jax import lax
from jax.experimental import pallas as pl
from jax.experimental.pallas import tpu as pltpu
from jax.sharding import PartitionSpec as P

MESH = pl.DeviceIdType.MESH
LANES = 128
MIB = 1024 * 1024
LATE_CHUNKS = (1, 6)
FIRST_CHUNKS = (1, 3)


def ordered_pieces(tile, shard_order):
    _, sub_count, row_count = shard_order.shape
    rows_tile, cols_tile = tile.shape
    piece_cols = cols_tile // row_count
    sub_cols = piece_cols // sub_count
    my_order = lax.dynamic_index_in_dim(shard_order, lax.axis_index("col"), 0, keepdims=False)
    blocks = tile.reshape(rows_tile, row_count, sub_count, sub_cols)
    pieces = []
    for s in range(row_count):
        piece = blocks[:, 0]
        for j in range(1, row_count):
            piece = jnp.where((my_order[:, s] == j)[None, :, None], blocks[:, j], piece)
        pieces.append(piece.reshape(rows_tile, piece_cols))
    return jnp.concatenate(pieces, axis=1)


def by_core(pair):
    return jnp.where(lax.rem(lax.axis_index("col"), 2) == 0, pair[0], pair[1])


def late_start(chunks, late):
    return chunks - by_core(late)


def row_tiles(cols):
    return 256 if cols % 256 == 0 else LANES


def step_of(rows):
    return 16 if rows % 16 == 0 else 8


def arrange_rows(order_ref, raw_ref, n_row, first, rows, reorder, shifts, place):
    r, c = lax.axis_index("row"), lax.axis_index("col")
    cols = raw_ref.shape[1] // n_row
    sub_count = order_ref.shape[2]
    sub_cols = cols // sub_count
    step = step_of(rows)

    @pl.loop(0, rows // step)
    def _(i):
        to = first + i * step
        at = pl.ds(pl.multiple_of(to, step), step)
        if reorder:
            for k in range(sub_count):
                blocks = [raw_ref[at, pl.ds(j * cols + k * sub_cols, sub_cols)] for j in range(n_row)]
                for t in shifts:
                    s = lax.rem(r + t, n_row)
                    piece = blocks[0]
                    for j in range(1, n_row):
                        piece = jnp.where(order_ref[c, s, k] == j, blocks[j], piece)
                    place(t, to, pl.ds(k * sub_cols, sub_cols), piece)
        else:
            for t in shifts:
                s = lax.rem(r + t, n_row)
                place(t, to, pl.ds(0, cols), raw_ref[at, pl.ds(pl.multiple_of(s * cols, LANES), cols)])


def edges(n_rep):
    z = lax.axis_index("rep")
    return z == n_rep - 2, z == 1, z == n_rep - 1, z == 0


def pair_barrier(n_rep, above, below):
    gives_up, gives_down, takes_below, takes_above = edges(n_rep)
    barrier = pltpu.get_barrier_semaphore()

    @pl.when(gives_up | takes_above)
    def _():
        pl.semaphore_signal(barrier, inc=1, device_id=above, device_id_type=MESH)

    @pl.when(gives_down | takes_below)
    def _():
        pl.semaphore_signal(barrier, inc=1, device_id=below, device_id_type=MESH)

    return barrier, (gives_up | takes_above).astype(jnp.int32) + (gives_down | takes_below).astype(jnp.int32)


def first_kernel(
    n_row, n_rep, chunks, first, reorder,
    order_hbm, tile_ref, landed_ref, order_ref, raw_ref, own_ref, order_sem, raw_sem, send_sem, recv_sem,
):
    r, c, z = lax.axis_index("row"), lax.axis_index("col"), lax.axis_index("rep")
    rows = tile_ref.shape[0] // chunks
    count = by_core(first)
    gives_up, gives_down, takes_below, takes_above = edges(n_rep)
    above = (r, c, jnp.minimum(z + 1, n_rep - 1))
    below = (r, c, jnp.maximum(z - 1, 0))
    barrier, expected = pair_barrier(n_rep, above, below)

    parts = 4 if rows % 64 == 0 else 1
    part = rows // parts

    def chunk_of(ref, q, i=None):
        if i is None:
            return ref.at[pl.ds(pl.multiple_of(q * rows, 8), rows)]
        return ref.at[pl.ds(pl.multiple_of(q * rows + i * part, 8), part)]

    def staged(q):
        return pltpu.make_async_copy(chunk_of(tile_ref, q), chunk_of(raw_ref, q), raw_sem.at[parts + q])

    def staged_part(i):
        return pltpu.make_async_copy(chunk_of(tile_ref, 0, i), chunk_of(raw_ref, 0, i), raw_sem.at[i])

    def moved(q, target, i=None):
        return pltpu.make_async_remote_copy(
            src_ref=chunk_of(own_ref, q, i),
            dst_ref=chunk_of(landed_ref, q, i),
            send_sem=send_sem.at[q],
            recv_sem=recv_sem.at[q],
            device_id=target,
            device_id_type=MESH,
        )

    def place(t, to, span, piece):
        own_ref[pl.ds(pl.multiple_of(to, 8), step_of(rows)), span] = piece

    gives = gives_up | gives_down

    def arrange(first, height):
        arrange_rows(order_ref, raw_ref, n_row, first, height, reorder, (0,), place)

    @pl.when(gives)
    def _():
        order_copy = pltpu.make_async_copy(order_hbm, order_ref, order_sem)
        order_copy.start()

        @pl.loop(0, parts)
        def _(i):
            staged_part(i).start()

        order_copy.wait()
        staged_part(0).wait()
        arrange(0, part)

        @pl.loop(1, count)
        def _(q):
            staged(q).start()

    @pl.when(expected > 0)
    def _():
        pl.semaphore_wait(barrier, expected)

    def send(q, i=None):
        @pl.when(gives_up)
        def _():
            moved(q, above, i).start()

        @pl.when(gives_down)
        def _():
            moved(q, below, i).start()

    @pl.when(gives)
    def _():
        send(0, 0)

        @pl.loop(1, parts)
        def _(i):
            staged_part(i).wait()
            arrange(i * part, part)

        @pl.loop(1, parts)
        def _(i):
            send(0, i)

        @pl.loop(1, count)
        def _(q):
            staged(q).wait()
            arrange(q * rows, rows)

        @pl.loop(1, count)
        def _(q):
            send(q)

        @pl.loop(0, count)
        def _(q):
            @pl.when(gives_up)
            def _():
                moved(q, above).wait_send()

            @pl.when(gives_down)
            def _():
                moved(q, below).wait_send()

    @pl.when(takes_below)
    def _():
        @pl.loop(0, count)
        def _(q):
            moved(q, below).wait_recv()

    @pl.when(takes_above)
    def _():
        @pl.loop(0, count)
        def _(q):
            moved(q, above).wait_recv()


def first_handoff(tile, order, cols, chunks, first, reorder):
    n_row, n_rep = lax.axis_size("row"), lax.axis_size("rep")
    slots = max(first)
    height = slots * (tile.shape[0] // chunks)
    dma = pltpu.SemaphoreType.DMA
    return pl.pallas_call(
        functools.partial(first_kernel, n_row, n_rep, chunks, first, reorder),
        out_shape=pltpu.VMEM((height, cols), tile.dtype),
        in_specs=[hbm(), hbm()],
        out_specs=vmem(),
        scratch_shapes=[
            pltpu.SMEM(order.shape, order.dtype),
            pltpu.VMEM((height, tile.shape[1]), tile.dtype),
            pltpu.VMEM((height, cols), tile.dtype),
            dma,
            dma((slots + 4,)),
            dma((slots,)),
            dma((slots,)),
        ],
        compiler_params=pltpu.CompilerParams(
            collective_id=2, has_side_effects=True, vmem_limit_bytes=6 * MIB
        ),
    )(in_hbm(order), in_hbm(tile))


def handoff_kernel(
    n_row, n_rep, chunks, late, first, reorder,
    order_hbm, tile_ref, hidden_hbm, landed_ref, full_ref, projected_ref, keep_ref,
    order_ref, raw_ref, away_ref, hidden_ref, order_sem, raw_sem, hidden_sem, y_send, y_recv, z_recv, up_send, down_send,
):
    r, c, z = lax.axis_index("row"), lax.axis_index("col"), lax.axis_index("rep")
    rows_tile, cols_tile = tile_ref.shape
    cols = cols_tile // n_row
    rows = rows_tile // chunks
    has_up, has_down = z < n_rep - 1, z > 0
    above = (r, c, jnp.minimum(z + 1, n_rep - 1))
    below = (r, c, jnp.maximum(z - 1, 0))
    per_level = n_row * chunks
    mine = z * n_row + r
    kept = (n_row - 1) * chunks + late_start(chunks, late)
    gives_up, gives_down, takes_below, takes_above = edges(n_rep)
    ahead = by_core(first)
    up_from, down_from = jnp.where(gives_up, ahead, 0), jnp.where(gives_down, ahead, 0)

    barrier = pltpu.get_barrier_semaphore()
    for t in range(1, n_row):
        pl.semaphore_signal(barrier, inc=1, device_id=(lax.rem(r + t, n_row), c, z), device_id_type=MESH)

    @pl.when(has_up)
    def _():
        pl.semaphore_signal(barrier, inc=1, device_id=above, device_id_type=MESH)

    @pl.when(has_down)
    def _():
        pl.semaphore_signal(barrier, inc=1, device_id=below, device_id_type=MESH)

    def chunk_of(ref, block, q):
        return ref.at[pl.ds(pl.multiple_of(block * rows_tile + q * rows, 8), rows)]

    def staged(q):
        return pltpu.make_async_copy(chunk_of(tile_ref, 0, q), chunk_of(raw_ref, 0, q), raw_sem.at[q])

    order_copy = pltpu.make_async_copy(order_hbm, order_ref, order_sem)
    hidden_copy = pltpu.make_async_copy(hidden_hbm, hidden_ref, hidden_sem)
    order_copy.start()
    staged(0).start()

    def place(t, to, span, piece):
        if t == 0:
            full_ref[pl.ds(pl.multiple_of(mine * rows_tile + to, 8), step), span] = piece
        else:
            away_ref[t - 1, pl.ds(pl.multiple_of(to, 8), step), span] = piece

    step = step_of(rows)

    def arrange(q):
        staged(q).wait()
        arrange_rows(order_ref, raw_ref, n_row, q * rows, rows, reorder, range(n_row), place)

    def along_row(t, q, outward):
        peer = lax.rem(r + t, n_row)
        source = lax.rem(r - t + n_row, n_row)
        return pltpu.make_async_remote_copy(
            src_ref=chunk_of(away_ref.at[t - 1], 0, q),
            dst_ref=chunk_of(full_ref, z * n_row + (r if outward else source), q),
            send_sem=y_send.at[t * chunks + q],
            recv_sem=y_recv.at[t * chunks + q],
            device_id=(peer, c, z),
            device_id_type=MESH,
        )

    def along_rep(block, q, sems, target):
        return pltpu.make_async_remote_copy(
            src_ref=chunk_of(full_ref, block, q),
            dst_ref=chunk_of(full_ref, block, q),
            send_sem=sems.at[block * chunks + q],
            recv_sem=z_recv.at[block * chunks + q],
            device_id=target,
            device_id_type=MESH,
        )

    def forward(block, q, up=True, down=True):
        @pl.when(has_up & up)
        def _():
            along_rep(block, q, up_send, above).start()

        @pl.when(has_down & down)
        def _():
            along_rep(block, q, down_send, below).start()

    by_chunk = rows % LANES == 0
    tile = row_tiles(cols)

    def multiply(first, depth, fresh):
        within = pl.ds(first, depth)

        @pl.loop(0, cols // tile)
        def _(n):
            at = pl.ds(pl.multiple_of(n * tile, tile), tile)
            term = jnp.dot(hidden_ref[:, within], full_ref[within, at], preferred_element_type=jnp.float32)
            projected_ref[:, at] = term if fresh else projected_ref[:, at] + term

    def consume(block, q):
        if by_chunk:
            multiply(pl.multiple_of(block * rows_tile + q * rows, LANES), rows, False)

    def send_own(q):
        forward(mine, q, q >= up_from, q >= down_from)
        for t in range(1, n_row):
            along_row(t, q, True).start()

    order_copy.wait()
    arrange(0)

    @pl.loop(1, chunks)
    def _(q):
        staged(q).start()

    hidden_copy.start()
    pl.semaphore_wait(barrier, n_row - 1 + has_up.astype(jnp.int32) + has_down.astype(jnp.int32))
    send_own(0)

    @pl.loop(1, chunks)
    def _(q):
        arrange(q)

        @pl.when(q > 1)
        def _():
            send_own(q - 1)

    if chunks > 1:
        send_own(chunks - 1)

    if by_chunk:
        projected_ref[...] = jnp.zeros_like(projected_ref)
    hidden_copy.wait()

    @pl.loop(0, chunks)
    def _(q):
        consume(mine, q)

    for t in range(1, n_row):

        @pl.loop(0, chunks)
        def _(q):
            along_row(t, q, False).wait_recv()
            block = z * n_row + lax.rem(r - t + n_row, n_row)
            forward(block, q)
            consume(block, q)

    def block_of(level, i):
        return level * n_row + lax.rem(r - i // chunks + n_row, n_row), lax.rem(i, chunks)

    def arrived(d, level, i, sems, target, onward):
        block, q = block_of(level, i)
        copy = along_rep(block, q, sems, target)
        taken = (d == 1) & (i < ahead) & jnp.logical_not(onward)

        @pl.when(jnp.logical_not(taken))
        def _():
            copy.wait_recv()

        if max(first):

            @pl.when(taken)
            def _():
                full_ref[pl.ds(pl.multiple_of(block * rows_tile + q * rows, LANES), rows), :] = landed_ref[
                    pl.ds(pl.multiple_of(jnp.minimum(q, max(first) - 1) * rows, LANES), rows), :
                ]

        deferred = (d == n_rep - 2) & (i >= kept)

        @pl.when(onward & jnp.logical_not(deferred))
        def _():
            copy.start()

        consume(block, q)
        if max(late):

            @pl.when(onward & deferred)
            def _():
                slot = q - (chunks - max(late))
                keep_ref[pl.ds(pl.multiple_of(slot * rows, LANES), rows), :] = full_ref[
                    pl.ds(pl.multiple_of(block * rows_tile + q * rows, LANES), rows), :
                ]

    @pl.loop(1, n_rep)
    def _(d):
        @pl.loop(0, per_level)
        def _(i):
            @pl.when(z - d >= 0)
            def _():
                @pl.when((d < n_rep - 1) | (i < kept))
                def _():
                    arrived(d, z - d, i, up_send, above, has_up)

            @pl.when(z + d < n_rep)
            def _():
                @pl.when((d < n_rep - 1) | (i < kept))
                def _():
                    arrived(d, z + d, i, down_send, below, has_down)

    if not by_chunk:
        multiply(0, full_ref.shape[0], True)

    @pl.loop(0, chunks)
    def _(q):
        for t in range(1, n_row):
            along_row(t, q, True).wait_send()

    def drain(level, begin, sent, sems, target):
        @pl.loop(begin, sent)
        def _(i):
            block, q = block_of(level, i)
            along_rep(block, q, sems, target).wait_send()

    @pl.when(has_up)
    def _():
        @pl.loop(0, z + 1)
        def _(level):
            drain(level, jnp.where(level == z, up_from, 0), jnp.where((level == 0) & gives_up, kept, per_level), up_send, above)

    @pl.when(has_down)
    def _():
        @pl.loop(z, n_rep)
        def _(level):
            drain(level, jnp.where(level == z, down_from, 0), jnp.where((level == n_rep - 1) & gives_down, kept, per_level), down_send, below)


def vmem():
    return pl.BlockSpec(memory_space=pltpu.VMEM)


def in_hbm(x):
    return pltpu.with_memory_space_constraint(x, pltpu.HBM)


def hbm():
    return pl.BlockSpec(memory_space=pltpu.HBM)


def handed_off(hidden, tile, order, chunks, late, first, reorder):
    n_row, n_rep = lax.axis_size("row"), lax.axis_size("rep")
    rows_tile, cols_tile = tile.shape
    cols = cols_tile // n_row
    every = n_rep * n_row * chunks
    if max(first):
        landed = first_handoff(tile, order, cols, chunks, first, reorder)
    else:
        landed = jnp.zeros((8, cols), tile.dtype)
    dma = pltpu.SemaphoreType.DMA
    height = n_rep * n_row * rows_tile
    return pl.pallas_call(
        functools.partial(handoff_kernel, n_row, n_rep, chunks, late, first, reorder),
        out_shape=(
            pltpu.VMEM((height, cols), tile.dtype),
            pltpu.VMEM((hidden.shape[0], cols), jnp.float32),
            pltpu.VMEM((max(8, max(late) * (rows_tile // chunks)), cols), tile.dtype),
        ),
        in_specs=[hbm(), hbm(), hbm(), vmem()],
        out_specs=(vmem(),) * 3,
        scratch_shapes=[
            pltpu.SMEM(order.shape, order.dtype),
            pltpu.VMEM((rows_tile, cols_tile), tile.dtype),
            pltpu.VMEM((n_row - 1, rows_tile, cols), tile.dtype),
            pltpu.VMEM(hidden.shape, hidden.dtype),
            dma,
            dma((chunks,)),
            dma,
            dma((n_row * chunks,)),
            dma((n_row * chunks,)),
            dma((every,)),
            dma((every,)),
            dma((every,)),
        ],
        compiler_params=pltpu.CompilerParams(
            collective_id=0, has_side_effects=True, vmem_limit_bytes=14 * MIB
        ),
    )(in_hbm(order), in_hbm(tile), in_hbm(hidden), landed)


def store_kernel(landed_ref, served_ref, sem):
    parts = sem.shape[0]
    rows = served_ref.shape[0] // parts
    copies = [
        pltpu.make_async_copy(
            landed_ref.at[pl.ds(i * rows, rows)], served_ref.at[pl.ds(i * rows, rows)], sem.at[i]
        )
        for i in range(parts)
    ]
    for copy in copies:
        copy.start()
    for copy in copies:
        copy.wait()


def stored(landed):
    return pl.pallas_call(
        store_kernel,
        out_shape=jax.ShapeDtypeStruct(landed.shape, landed.dtype),
        in_specs=[pl.BlockSpec(memory_space=pl.ANY)],
        out_specs=pl.BlockSpec(memory_space=pl.ANY),
        scratch_shapes=[pltpu.SemaphoreType.DMA((8,))],
        compiler_params=pltpu.CompilerParams(vmem_limit_bytes=MIB),
    )(landed)


def late_kernel(
    n_row, n_rep, chunks, late,
    keep_ref, partial_ref, hidden_hbm, _, late_ref, summed_ref,
    hidden_ref, hidden_sem, send_sem, recv_sem,
):
    r, c, z = lax.axis_index("row"), lax.axis_index("col"), lax.axis_index("rep")
    slots = max(late)
    rows, cols = late_ref.shape[0] // slots, late_ref.shape[1]
    first = late_start(chunks, late)
    other = lax.rem(r + 1, n_row)
    lowest, highest = other, (n_rep - 1) * n_row + other
    gives_up, gives_down, takes_below, takes_above = edges(n_rep)
    above = (r, c, jnp.minimum(z + 1, n_rep - 1))
    below = (r, c, jnp.maximum(z - 1, 0))

    barrier, expected = pair_barrier(n_rep, above, below)
    pl.semaphore_wait(barrier, expected)

    def moved(q, target):
        slot = q - (chunks - slots)
        return pltpu.make_async_remote_copy(
            src_ref=keep_ref.at[pl.ds(pl.multiple_of(slot * rows, LANES), rows)],
            dst_ref=late_ref.at[pl.ds(pl.multiple_of(slot * rows, LANES), rows)],
            send_sem=send_sem.at[slot],
            recv_sem=recv_sem.at[slot],
            device_id=target,
            device_id_type=MESH,
        )

    @pl.when(gives_up)
    def _():
        @pl.loop(first, chunks)
        def _(q):
            moved(q, above).start()

    @pl.when(gives_down)
    def _():
        @pl.loop(first, chunks)
        def _(q):
            moved(q, below).start()

    summed_ref[...] = partial_ref[...]
    tile = row_tiles(cols)

    def take(block, target):
        hidden_copy = pltpu.make_async_copy(
            hidden_hbm.at[:, pl.ds(pl.multiple_of((block * chunks + chunks - slots) * rows, LANES), slots * rows)],
            hidden_ref,
            hidden_sem,
        )
        hidden_copy.start()
        hidden_copy.wait()

        @pl.loop(first, chunks)
        def _(q):
            moved(q, target).wait_recv()
            within = pl.ds(pl.multiple_of((q - (chunks - slots)) * rows, LANES), rows)
            for n in range(cols // tile):
                at = pl.ds(n * tile, tile)
                summed_ref[:, at] += jnp.dot(
                    hidden_ref[:, within], late_ref[within, at], preferred_element_type=jnp.float32
                )

    @pl.when(takes_below)
    def _():
        take(lowest, below)

    @pl.when(takes_above)
    def _():
        take(highest, above)

    @pl.when(gives_up)
    def _():
        @pl.loop(first, chunks)
        def _(q):
            moved(q, above).wait_send()

    @pl.when(gives_down)
    def _():
        @pl.loop(first, chunks)
        def _(q):
            moved(q, below).wait_send()


def late_handoff(keep, partial, hidden, token, chunks, late):
    n_row, n_rep = lax.axis_size("row"), lax.axis_size("rep")
    slots = max(late)
    rows = keep.shape[0] // slots
    dma = pltpu.SemaphoreType.DMA
    return pl.pallas_call(
        functools.partial(late_kernel, n_row, n_rep, chunks, late),
        out_shape=(
            pltpu.VMEM(keep.shape, keep.dtype),
            pltpu.VMEM(partial.shape, partial.dtype),
        ),
        in_specs=[vmem(), vmem(), hbm(), hbm()],
        out_specs=(vmem(), vmem()),
        scratch_shapes=[
            pltpu.VMEM((hidden.shape[0], slots * rows), hidden.dtype),
            dma,
            dma((slots,)),
            dma((slots,)),
        ],
        cost_estimate=pl.CostEstimate(flops=10**11, bytes_accessed=10**6, transcendentals=0),
        compiler_params=pltpu.CompilerParams(
            collective_id=1, has_side_effects=True, vmem_limit_bytes=2 * MIB
        ),
    )(keep, partial, in_hbm(hidden), in_hbm(token))


def finish_kernel(n_row, n_rep, chunks, late, early_ref, late_ref, summed_ref, served_ref, projected_ref, sem, projected_sem):
    r, z = lax.axis_index("row"), lax.axis_index("rep")
    rows_tile = served_ref.shape[0] // (n_row * n_rep)
    rows = rows_tile // chunks
    slots = late_ref.shape[0] // rows
    first = late_start(chunks, late)
    block = jnp.where(z == 0, n_rep - 1, 0) * n_row + lax.rem(r + 1, n_row)
    takes = (z == 0) | (z == n_rep - 1)

    def stored(q):
        slot = q - (chunks - slots)
        return pltpu.make_async_copy(
            late_ref.at[pl.ds(pl.multiple_of(slot * rows, LANES), rows)],
            served_ref.at[pl.ds(pl.multiple_of(block * rows_tile + q * rows, LANES), rows)],
            sem.at[slot],
        )

    projected_copy = pltpu.make_async_copy(summed_ref, projected_ref, projected_sem)
    projected_copy.start()

    @pl.when(takes)
    def _():
        @pl.loop(first, chunks)
        def _(q):
            stored(q).start()

        @pl.loop(first, chunks)
        def _(q):
            stored(q).wait()

    projected_copy.wait()


def finished(early, landed, summed, chunks, late):
    n_row, n_rep = lax.axis_size("row"), lax.axis_size("rep")
    dma = pltpu.SemaphoreType.DMA
    return pl.pallas_call(
        functools.partial(finish_kernel, n_row, n_rep, chunks, late),
        out_shape=(
            jax.ShapeDtypeStruct(early.shape, early.dtype),
            jax.ShapeDtypeStruct(summed.shape, summed.dtype),
        ),
        in_specs=[pl.BlockSpec(memory_space=pl.ANY), vmem(), vmem()],
        out_specs=(pl.BlockSpec(memory_space=pl.ANY),) * 2,
        scratch_shapes=[dma((max(late),)), dma],
        input_output_aliases={0: 0},
        compiler_params=pltpu.CompilerParams(vmem_limit_bytes=MIB),
    )(early, landed, summed)


def shards(hidden, train_weight, shard_order):
    _, sub_count, n_row = shard_order.shape
    rows_tile, cols_tile = train_weight.shape
    chunks = rows_tile // LANES if rows_tile % LANES == 0 else 1
    split = chunks > max(LATE_CHUNKS + FIRST_CHUNKS) and lax.axis_size("rep") > 3
    late = LATE_CHUNKS if split else (0, 0)
    first = FIRST_CHUNKS if split else (0, 0)
    reorder = (cols_tile // (n_row * sub_count)) % LANES == 0
    tile = train_weight if reorder else ordered_pieces(train_weight, shard_order)
    landed, summed, keep = handed_off(hidden, tile, jnp.swapaxes(shard_order, 1, 2), chunks, late, first, reorder)
    served = stored(landed)
    if max(late) == 0:
        return served, summed
    tail, total = late_handoff(keep, summed, hidden, served, chunks, late)
    return finished(served, tail, total, chunks, late)


def solution(mesh):
    placed = (P("rep", None), P(("rep", "row"), "col"), P())
    return jax.shard_map(
        shards,
        mesh=mesh,
        in_specs=placed,
        out_specs=(P(None, ("col", "row")), P("rep", ("col", "row"))),
        check_vma=False,
    )
```
